32 devices in a mesh: dp: 8 (over y, x, core), tile: 4 (over z).
Axes of the slice: x: 2, y: 2, z: 4, core: 2. Of those that a mesh axis runs over, the one named last changes fastest.
Arguments:
- frames: bfloat16 [4, 3, 16, 16, 1024], P('tile', None, None, None, 'dp'), may hold values from -9 to 9
- weights: bfloat16 [4, 64, 8, 972], P('tile'), may hold values from -0.1875 to 0.1875
- connect: int32 [4, 64, 8, 3], P('tile'), may hold values 0 or 1
Outputs:
- update: bfloat16 [4, 64, 8, 972], P('tile')
- loss_value: float32 [], replicated
The draws below stay inside these ranges and needn't reach their ends.
All inputs are finite; a program needn't handle non-finite values. No bound on the sum of `connect` on one device may be relied on, other than what follows from the above.
Results may differ from the reference program's by a relative error of at most 0.008.
Values may be sent and summed in bfloat16 or wider, within the bound.
No kernel may reach another device: no remote copies, remote signals or barrier semaphores. Data moves between devices by JAX's collectives and lax.ppermute only.
A program may use at most 64 MiB of HBM per device.

```python
import jax
import jax.numpy as jnp
from jax import lax

FIELD = 18
MAPS = 8
STRIDE = 2
TILE_PX = 16
INPUTS = 972
HALO = 16
POS = 64
SIDE = 2
TILES = 4
BATCH = 1024


def draw_frames(key, part):
    subkeys = jax.random.split(jax.random.fold_in(key, 17), 3)
    shape = (TILES, 3, TILE_PX, TILE_PX, BATCH)
    tile_ids = jnp.arange(TILES).reshape(TILES, 1, 1, 1, 1)
    row_pos = jnp.arange(TILE_PX).reshape(1, 1, TILE_PX, 1, 1)
    col_pos = jnp.arange(TILE_PX).reshape(1, 1, 1, TILE_PX, 1)
    frame_pos = jnp.arange(BATCH).reshape(1, 1, 1, 1, BATCH)
    global_row = tile_ids // SIDE * TILE_PX + row_pos
    global_col = tile_ids % SIDE * TILE_PX + col_pos
    extent = SIDE * TILE_PX
    trend = 3.0 ** ((global_row + global_col).astype(jnp.float32) / (2.0 * extent) + frame_pos.astype(jnp.float32) / BATCH)
    rough = jax.random.uniform(subkeys[0], shape, jnp.float32, 0.6, 1.4)
    base = jnp.clip(jax.random.normal(subkeys[2], shape, jnp.float32), -2.0, 2.0)
    return (0.35 * trend * rough * base).astype(jnp.bfloat16)


def with_ends(entries, key, least, largest):
    shape = entries.shape
    spot = [jax.random.randint(jax.random.fold_in(key, axis), (), 0, shape[axis]) for axis in range(len(shape))]
    entries = entries.at[tuple(spot)].set(least)
    longest = shape.index(max(shape))
    spot[longest] = (spot[longest] + 1) % shape[longest]
    return entries.at[tuple(spot)].set(largest)


def block_scale(own_key, dims, shards, smallest, top_value):
    factor_of = 1.0
    for dim, blocks in shards:
        heights = jax.random.uniform(jax.random.fold_in(jax.random.fold_in(own_key, 6), dim), (blocks,), jnp.float32, smallest / len(shards), top_value / len(shards))
        factor_of = factor_of * jnp.repeat(jnp.exp(heights), dims[dim] // blocks).reshape((-1,) + (1,) * (len(dims) - 1 - dim))
    return factor_of


def normal_values(own_key, shape, deviation, reach, shards=(), kind=jnp.bfloat16):
    values = deviation * jax.random.normal(own_key, shape, jnp.float32)
    if shards:
        values = values * block_scale(own_key, shape, shards, -0.22, 0.18)
    return jnp.clip(values, -reach, reach).astype(kind)


def setup_inputs(seed: int = 0) -> dict:
    streams_of = jax.random.split(jax.random.key(seed), 4)
    return {
        "frames": draw_frames(jax.random.fold_in(streams_of[3], 71), 0),
        "weights": normal_values(streams_of[1], (TILES, POS, MAPS, INPUTS), INPUTS ** -0.5, 0.1875, ((0, 4),)),
        "connect": with_ends((jax.random.randint(streams_of[2], (TILES, POS, MAPS, 3), 0, 4) < 3).astype(jnp.int32), jax.random.fold_in(streams_of[2], 1), 0, 1),
    }


sparsity_weight = 1.0
smooth_eps = 0.01
guard_eps = 1e-06

def masked(values, connect):
    blocked = values.reshape(values.shape[0], POS, MAPS, 3, FIELD * FIELD)
    opened = connect.astype(values.dtype)[..., None]
    return (blocked * opened).reshape(values.shape)

def patch_block(extended, row_index):
    strip_rows = lax.dynamic_slice_in_dim(extended, (row_index * STRIDE).astype(jnp.int32), FIELD, 1)
    pieces = [strip_rows[:, :, column * STRIDE:column * STRIDE + FIELD] for column in range(TILE_PX // STRIDE)]
    blocks = jnp.stack(pieces, 0)
    return blocks.reshape(blocks.shape[0], INPUTS, blocks.shape[-1])

def spread(coeffs, span_px):
    shaped = coeffs.reshape(coeffs.shape[0], 3, FIELD, FIELD, coeffs.shape[-1])
    canvas_strip = jnp.zeros((3, FIELD, span_px, coeffs.shape[-1]), jnp.float32)
    for column in range(TILE_PX // STRIDE):
        canvas_strip = canvas_strip.at[:, :, column * STRIDE:column * STRIDE + FIELD].add(shaped[column])
    return canvas_strip

def neighbour_ids(tile_index):
    right_id = ((tile_index + 1) % TILES).astype(jnp.int32)
    below_id = ((tile_index + SIDE) % TILES).astype(jnp.int32)
    corner_id = ((tile_index + SIDE + 1) % TILES).astype(jnp.int32)
    return (right_id, below_id, corner_id)

def pick_tile(stack, index):
    return lax.dynamic_index_in_dim(stack, index.astype(jnp.int32), 0, keepdims=False)

def extended_tile(stack, tile_index):
    right_id, below_id, corner_id = neighbour_ids(tile_index)
    upper = jnp.concatenate([pick_tile(stack, tile_index), pick_tile(stack, right_id)[:, :, :HALO]], axis=2)
    lower = jnp.concatenate([pick_tile(stack, below_id)[:, :HALO], pick_tile(stack, corner_id)[:, :HALO, :HALO]], axis=2)
    return jnp.concatenate([upper, lower], axis=1)

def add_region(canvas, index, row_lo, col_lo, piece):
    current = pick_tile(canvas, index)
    current = current.at[:, row_lo:row_lo + piece.shape[1], col_lo:col_lo + piece.shape[2]].add(piece)
    return lax.dynamic_update_index_in_dim(canvas, current, index.astype(jnp.int32), 0)

def reference(frames, weights, connect):
    frames_total = frames.shape[-1]
    rows_out = TILE_PX // STRIDE
    span_px = TILE_PX + HALO
    effective = masked(weights, connect).reshape(TILES, rows_out, rows_out, MAPS, INPUTS)

    def encode_tile(canvas, tile_index):
        extended = extended_tile(frames, tile_index)
        weight_rows = effective[tile_index]

        def row_step(canvas_part, row_index):
            blocks = patch_block(extended, row_index)
            w_row = weight_rows[row_index].astype(jnp.float32)
            coded = jnp.einsum('cmk,ckb->cmb', w_row, blocks.astype(jnp.float32))
            rounded = coded.astype(jnp.bfloat16).astype(jnp.float32)
            decoded = jnp.einsum('cmk,cmb->ckb', w_row, rounded)
            start = (row_index * STRIDE).astype(jnp.int32)
            window = lax.dynamic_slice_in_dim(canvas_part, start, FIELD, 1)
            canvas_part = lax.dynamic_update_slice_in_dim(canvas_part, window + spread(decoded, span_px), start, 1)
            return (canvas_part, coded)
        canvas_part, coded = lax.scan(row_step, jnp.zeros((3, span_px, span_px, frames_total), jnp.float32), jnp.arange(rows_out, dtype=jnp.int32))
        right_id, below_id, corner_id = neighbour_ids(tile_index)
        canvas = add_region(canvas, tile_index, 0, 0, canvas_part[:, :TILE_PX, :TILE_PX])
        canvas = add_region(canvas, right_id, 0, 0, canvas_part[:, :TILE_PX, TILE_PX:])
        canvas = add_region(canvas, below_id, 0, 0, canvas_part[:, TILE_PX:, :TILE_PX])
        canvas = add_region(canvas, corner_id, 0, 0, canvas_part[:, TILE_PX:, TILE_PX:])
        return (canvas, coded)
    canvas, coded_all = lax.scan(encode_tile, jnp.zeros((TILES, 3, TILE_PX, TILE_PX, frames_total), jnp.float32), jnp.arange(TILES, dtype=jnp.int32))
    errors = canvas - frames.astype(jnp.float32)
    error_sq = jnp.sum(errors * errors)
    sparse = jnp.sum(jnp.sqrt(smooth_eps + coded_all * coded_all))
    error_tiles = errors.astype(jnp.bfloat16)

    def grad_tile(unused, inputs):
        tile_index, coded_tile = inputs
        ext_frames = extended_tile(frames, tile_index)
        ext_errors = extended_tile(error_tiles, tile_index)
        weight_rows = effective[tile_index]

        def row_step(inner, pair):
            row_index, coded = pair
            frame_block = patch_block(ext_frames, row_index).astype(jnp.float32)
            error_block = patch_block(ext_errors, row_index).astype(jnp.float32)
            w_row = weight_rows[row_index].astype(jnp.float32)
            encoded_err = jnp.einsum('cmk,ckb->cmb', w_row, error_block)
            left_coef = (2.0 * coded).astype(jnp.bfloat16).astype(jnp.float32)
            right_coef = (2.0 * encoded_err + sparsity_weight * coded / jnp.sqrt(smooth_eps + coded * coded)).astype(jnp.bfloat16).astype(jnp.float32)
            grad_row = jnp.einsum('cmb,ckb->cmk', left_coef, error_block) + jnp.einsum('cmb,ckb->cmk', right_coef, frame_block)
            return (inner, grad_row)
        inner, grad_rows = lax.scan(row_step, unused, (jnp.arange(rows_out, dtype=jnp.int32), coded_tile))
        return (inner, grad_rows.reshape(POS, MAPS, INPUTS))
    unused, gradients = lax.scan(grad_tile, jnp.zeros((), jnp.float32), (jnp.arange(TILES, dtype=jnp.int32), coded_all))
    gradients = masked(gradients, connect)
    mean_sq = jnp.sum(gradients * gradients) / (TILES * POS * MAPS * INPUTS)
    update = (-(gradients * lax.rsqrt(mean_sq + guard_eps))).astype(jnp.bfloat16)
    loss_value = ((error_sq + sparsity_weight * sparse) / frames_total).astype(jnp.float32)
    return (update, loss_value)
```

```python
import math

import jax
import jax.numpy as jnp
from jax import lax
from jax.experimental import pallas as pl
from jax.experimental.pallas import tpu as pltpu
from jax.sharding import PartitionSpec as P

FIELD = 18
MAPS = 8
STRIDE = 2
TILE_PX = 16
INPUTS = 972
HALO = 16
POS = 64
SPAN = TILE_PX + HALO
SIDE_POS = TILE_PX // STRIDE
UNITS = POS * MAPS
PLANE = SPAN * SPAN
PATCH = FIELD * FIELD
LANES = 128
PAD_IN = -(-INPUTS // LANES) * LANES
STRIP = FIELD * SPAN
PAD_STRIP = -(-STRIP // LANES) * LANES
ROLL_W = PAD_STRIP + LANES
GRAB = 512
STEP_IN = 256

sparsity_weight = 1.0
smooth_eps = 0.01
guard_eps = 1e-06

BF = jnp.bfloat16
F32 = jnp.float32
VMEM_CAP = 40 * 1024 * 1024


def shift_by(value, axis, steps):
    count = lax.axis_size(axis)
    return lax.ppermute(value, axis, [(s, (s + steps) % count) for s in range(count)])


def swap_with(value, axis, flip):
    count = lax.axis_size(axis)
    return lax.ppermute(value, axis, [(s, s ^ flip) for s in range(count)])


def kernel_call(body, outs, scratch=(), scalars=0, n_in=0, flops=0, name=None):
    return pl.pallas_call(
        body,
        out_shape=outs,
        in_specs=[pl.BlockSpec(memory_space=pltpu.SMEM)] * scalars
        + [pl.BlockSpec(memory_space=pltpu.VMEM)] * n_in,
        out_specs=jax.tree.map(lambda _: pl.BlockSpec(memory_space=pltpu.VMEM), outs),
        scratch_shapes=list(scratch),
        compiler_params=pltpu.CompilerParams(vmem_limit_bytes=VMEM_CAP),
        cost_estimate=pl.CostEstimate(flops=flops, transcendentals=0, bytes_accessed=flops // 256),
        name=name,
    )


def positions():
    for i in range(SIDE_POS):
        for j in range(0, SIDE_POS, 2):
            lead = (i * STRIDE * SPAN) // LANES * LANES
            rest = i * STRIDE * SPAN - lead
            shifts = [rest + STRIDE * j, rest + STRIDE * (j + 1)]
            yield (i * SIDE_POS + j) * MAPS, lead, shifts


def place(dst, a, b, c, d):
    for ch in range(3):
        dst[ch, :TILE_PX, :TILE_PX] = a[ch]
        dst[ch, :TILE_PX, TILE_PX:] = b[ch]
        dst[ch, TILE_PX:, :TILE_PX] = c[ch]
        dst[ch, TILE_PX:, TILE_PX:] = d[ch]


def expand_body(w_ref, con_ref, wd_ref, wt_ref, wp_ref, v_ref, s_ref):
    wp_ref[:, PAD_IN - LANES :] = jnp.zeros((UNITS, LANES), BF)
    wp_ref[:, :INPUTS] = w_ref[...]
    n = lax.broadcasted_iota(jnp.int32, (1, PAD_STRIP), 1)
    row, col = n // SPAN, n % SPAN
    inside = (col < FIELD) & (row < FIELD)
    k = lax.broadcasted_iota(jnp.int32, (GRAB, PAD_STRIP), 0)
    v_ref[:, PAD_STRIP:] = jnp.zeros((UNITS, LANES), F32)
    for ch in range(3):
        want = jnp.where(inside, row * FIELD + col + ch * (PATCH - STEP_IN), -1)
        s_ref[...] = jnp.where(k == want, 1.0, 0.0).astype(BF)
        v = jnp.dot(
            wp_ref[:, ch * STEP_IN : ch * STEP_IN + GRAB], s_ref[...], preferred_element_type=F32
        )
        v_ref[:, :PAD_STRIP] = v * con_ref[:, ch : ch + 1]
        base = ch * PLANE
        for u, lead, shifts in positions():
            parts = []
            for h, s in enumerate(shifts):
                blk = v_ref[u + h * MAPS : u + (h + 1) * MAPS, :]
                parts.append(pltpu.roll(blk, s, 1) if s else blk)
            both = jnp.concatenate(parts, 0).astype(BF)
            width = min(ROLL_W, PLANE - lead)
            rows = slice(u, u + 2 * MAPS)
            if lead:
                wd_ref[rows, base : base + lead] = jnp.zeros((2 * MAPS, lead), BF)
            wd_ref[rows, base + lead : base + lead + width] = both[:, :width]
            left = PLANE - lead - width
            if left:
                wd_ref[rows, base + PLANE - left : base + PLANE] = jnp.zeros((2 * MAPS, left), BF)
        for kb in range(base, base + PLANE, LANES):
            wt_ref[kb : kb + LANES, :] = wd_ref[:, kb : kb + LANES].T


def encode_body(x0, x1, x2, x3, wd_ref, wt_ref, coded_ref, own_ref, r_ref, b_ref, c_ref, sp_ref, xe):
    place(xe, x0, x1, x2, x3)
    batch = x0.shape[-1]
    coded = jnp.dot(wd_ref[...], xe[...].reshape(3 * PLANE, batch), preferred_element_type=F32)
    coded_ref[...] = coded
    sparse = jnp.sqrt(smooth_eps + coded * coded)
    sp_ref[...] = jnp.sum(sparse.reshape(UNITS // 8, 8, batch), 0)
    rounded = coded.astype(BF)
    half = PLANE // 2
    for ch in range(3):
        for low in range(2):
            at = ch * PLANE + low * half
            part = jnp.dot(wt_ref[at : at + half, :], rounded, preferred_element_type=F32)
            part = part.reshape(TILE_PX, SPAN, batch)
            if low:
                b_ref[ch] = part[:, :TILE_PX].astype(BF)
                c_ref[ch] = part[:, TILE_PX:].astype(BF)
            else:
                own_ref[ch] = part[:, :TILE_PX]
                r_ref[ch] = part[:, TILE_PX:].astype(BF)


def error_body(own, fr, fb, fc, x, sp, e_ref, loss_ref):
    batch = x.shape[-1]
    total = sp[...] * sparsity_weight
    for ch in range(3):
        err = own[ch] + fr[ch].astype(F32) + fb[ch].astype(F32) + fc[ch].astype(F32)
        err = err - x[ch].astype(F32)
        e_ref[ch] = err.astype(BF)
        total = total + jnp.sum((err * err).reshape(TILE_PX * TILE_PX // 8, 8, batch), 0)
    loss_ref[...] = total


def grad_body(
    half_ref, wd_ref, coded_ref, x0, x1, x2, x3, e0, e1, e2, e3, con_ref,
    keep_ref, send_ref, ex, lr, gd, gs, st, out,
):
    batch = x0.shape[-1]
    place(ex.at[:, :, :, :batch], e0, e1, e2, e3)
    place(ex.at[:, :, :, batch:], x0, x1, x2, x3)
    e_all = ex[:, :, :, :batch].reshape(3 * PLANE, batch)
    enc = jnp.dot(wd_ref[...], e_all, preferred_element_type=F32)
    coded = coded_ref[...]
    lr[:, :batch] = (2.0 * coded).astype(BF)
    right = 2.0 * enc + sparsity_weight * coded / jnp.sqrt(smooth_eps + coded * coded)
    lr[:, batch:] = right.astype(BF)
    n = lax.broadcasted_iota(jnp.int32, (PAD_STRIP, 1), 0)
    row, col = n // SPAN, n % SPAN
    inside = (col < FIELD) & (row < FIELD)
    k = lax.broadcasted_iota(jnp.int32, (PAD_STRIP, GRAB), 1)
    out[...] = jnp.zeros((UNITS, PAD_IN), F32)
    for ch in range(3):
        pixels = ex[ch].reshape(PLANE, 2 * batch)
        gd[...] = lax.dot_general(
            lr[...], pixels, (((1,), (1,)), ((), ())), preferred_element_type=F32
        )
        want = jnp.where(inside, row * FIELD + col + ch * (PATCH - STEP_IN), -1)
        st[...] = jnp.where(k == want, 1.0, 0.0).astype(BF)
        for u, lead, shifts in positions():
            width = min(ROLL_W, PLANE - lead)
            parts = []
            for h, s in enumerate(shifts):
                blk = gd[u + h * MAPS : u + (h + 1) * MAPS, lead : lead + width]
                blk = pltpu.roll(blk, width - s, 1) if s else blk
                parts.append(blk[:, :PAD_STRIP])
            gs[u : u + 2 * MAPS, :] = jnp.concatenate(parts, 0).astype(BF)
        cols = slice(ch * STEP_IN, ch * STEP_IN + GRAB)
        out[:, cols] = out[:, cols] + jnp.dot(gs[...], st[...], preferred_element_type=F32)
    lane = lax.broadcasted_iota(jnp.int32, (1, PAD_IN), 1)
    con = con_ref[...]
    opened = jnp.where(
        lane < PATCH, con[:, 0:1], jnp.where(lane < 2 * PATCH, con[:, 1:2], con[:, 2:3])
    )
    out[...] = out[...] * opened
    rows = UNITS // 2
    mine = pl.multiple_of(half_ref[0] * rows, rows)
    other = pl.multiple_of((1 - half_ref[0]) * rows, rows)
    keep_ref[...] = out[pl.ds(mine, rows), :]
    send_ref[...] = out[pl.ds(other, rows), :].astype(BF)


def pair_body(chip_ref, keep, got, *refs):
    own_ref, sends, scr = refs[0], refs[1:-1], refs[-1]
    rows = own_ref.shape[0]
    scr[...] = keep[...] + got[...].astype(F32)
    chip = chip_ref[0]
    own_ref[...] = scr[pl.ds(pl.multiple_of(chip * rows, rows), rows), :]
    for x, ref in enumerate(sends):
        at = pl.multiple_of((chip ^ (x + 1)) * rows, rows)
        ref[...] = scr[pl.ds(at, rows), :].astype(BF)


def shard_body(own, *refs):
    got, loss, shard_ref, tally_ref = refs[:-3], refs[-3], refs[-2], refs[-1]
    total = own[...]
    for ref in got:
        total = total + ref[...].astype(F32)
    shard_ref[...] = total.astype(BF)
    rows, width = total.shape
    sq = jnp.sum((total * total).reshape(rows // 8, 8, width), 0)
    folded = sq[:, :LANES]
    for at in range(LANES, width, LANES):
        folded = folded + sq[:, at : at + LANES]
    tally_ref[:8] = loss[...]
    tally_ref[8:] = folded


def gather_body(chip_ref, own, *refs):
    got, half_ref = refs[:-1], refs[-1]
    rows = own.shape[0]
    chip = chip_ref[0]
    half_ref[pl.ds(pl.multiple_of(chip * rows, rows), rows), :] = own[...]
    for x, ref in enumerate(got):
        at = pl.multiple_of((chip ^ (x + 1)) * rows, rows)
        half_ref[pl.ds(at, rows), :] = ref[...]


def finish_body(entries, frames_total, half_ref, mine, other, ta, tb, up_ref, loss_ref):
    tally = ta[...] + tb[...]
    square = jnp.sum(jnp.sum(tally[8:], 0, keepdims=True), 1, keepdims=True)
    factor = lax.rsqrt(square / entries + guard_eps)
    rows = mine.shape[0]
    at = pl.multiple_of(half_ref[0] * rows, rows)
    up_ref[pl.ds(at, rows), :] = (-(mine[:, :INPUTS].astype(F32) * factor)).astype(BF)
    at = pl.multiple_of((1 - half_ref[0]) * rows, rows)
    up_ref[pl.ds(at, rows), :] = (-(other[:, :INPUTS].astype(F32) * factor)).astype(BF)
    loss = jnp.sum(jnp.sum(tally[:8], 0, keepdims=True), 1, keepdims=True) / frames_total
    loss_ref[...] = jnp.broadcast_to(loss, loss_ref.shape)


def local(frames, weights, connect):
    batch = frames.shape[-1]
    n_tile = lax.axis_size("tile")
    n_dp = lax.axis_size("dp")
    side = math.isqrt(n_tile)
    chips = n_dp // 2
    index = lax.axis_index("dp")
    core = (index % 2).astype(jnp.int32).reshape(1)
    chip = (index // 2).astype(jnp.int32).reshape(1)
    sds = jax.ShapeDtypeStruct
    dense_flops = 2 * UNITS * 3 * PLANE * batch

    x0 = frames[0]
    steps = (1, side, side + 1)
    xs = [shift_by(x0, "tile", -s) for s in steps]

    con = connect.reshape(UNITS, 3).astype(F32)
    wd, wt = kernel_call(
        expand_body,
        (sds((UNITS, 3 * PLANE), BF), sds((3 * PLANE, UNITS), BF)),
        [pltpu.VMEM((UNITS, PAD_IN), BF), pltpu.VMEM((UNITS, ROLL_W), F32), pltpu.VMEM((GRAB, PAD_STRIP), BF)],
        n_in=2, flops=4 * dense_flops, name="expand",
    )(weights.reshape(UNITS, INPUTS), con)

    quad = (3, TILE_PX, TILE_PX, batch)
    coded, own, sr, sb, sc, sparse = kernel_call(
        encode_body,
        (sds((UNITS, batch), F32), sds(quad, F32), sds(quad, BF), sds(quad, BF), sds(quad, BF), sds((8, batch), F32)),
        [pltpu.VMEM((3, SPAN, SPAN, batch), BF)],
        n_in=6, flops=2 * dense_flops, name="encode",
    )(x0, *xs, wd, wt)

    back = [shift_by(v, "tile", s) for v, s in zip((sr, sb, sc), steps)]
    e0, loss_part = kernel_call(
        error_body, (sds(quad, BF), sds((8, batch), F32)), n_in=6, flops=dense_flops // 8, name="errors"
    )(own, *back, x0, sparse)
    es = [shift_by(e0, "tile", -s) for s in steps]

    half = UNITS // 2
    keep, send = kernel_call(
        grad_body,
        (sds((half, PAD_IN), F32), sds((half, PAD_IN), BF)),
        [
            pltpu.VMEM((3, SPAN, SPAN, 2 * batch), BF),
            pltpu.VMEM((UNITS, 2 * batch), BF),
            pltpu.VMEM((UNITS, PLANE), F32),
            pltpu.VMEM((UNITS, PAD_STRIP), BF),
            pltpu.VMEM((PAD_STRIP, GRAB), BF),
            pltpu.VMEM((UNITS, PAD_IN), F32),
        ],
        scalars=1, n_in=11, flops=4 * dense_flops, name="grads",
    )(core, wd, coded, x0, *xs, e0, *es, con)

    got = swap_with(send, "dp", 1)
    rows = half // chips
    shard = sds((rows, PAD_IN), BF)
    split = kernel_call(
        pair_body,
        (sds((rows, PAD_IN), F32),) + (shard,) * (chips - 1),
        [pltpu.VMEM((half, PAD_IN), F32)],
        scalars=1, n_in=2, flops=dense_flops // 8, name="pair",
    )(chip, keep, got)
    arrived = [swap_with(v, "dp", 2 * (x + 1)) for x, v in enumerate(split[1:])]
    mine, tally = kernel_call(
        shard_body, (shard, sds((16, LANES), F32)), n_in=chips + 1, flops=dense_flops // 16, name="shard"
    )(split[0], *arrived, loss_part)

    others = [swap_with(mine, "dp", 2 * x) for x in range(1, chips)]
    tally = tally + sum(shift_by(tally, "tile", s) for s in range(1, n_tile))
    tally = tally + sum(swap_with(tally, "dp", 2 * x) for x in range(1, chips))
    tally_b = swap_with(tally, "dp", 1)
    mine_half = kernel_call(
        gather_body, sds((half, PAD_IN), BF), scalars=1, n_in=chips, flops=dense_flops // 16, name="gather"
    )(chip, mine, *others)
    other_half = swap_with(mine_half, "dp", 1)

    entries = n_tile * POS * MAPS * INPUTS
    update, loss = kernel_call(
        lambda *refs: finish_body(float(entries), float(batch * n_dp), *refs),
        (sds((UNITS, INPUTS), BF), sds((8, LANES), F32)),
        scalars=1, n_in=4, flops=dense_flops // 8, name="finish",
    )(core, mine_half, other_half, tally, tally_b)
    return update.reshape(1, POS, MAPS, INPUTS), loss[0, 0]


def solution(mesh):
    placed = (
        P("tile", None, None, None, "dp"),
        P("tile", None, None, None),
        P("tile", None, None, None),
    )
    return jax.shard_map(
        local,
        mesh=mesh,
        in_specs=placed,
        out_specs=(P("tile", None, None, None), P()),
        check_vma=False,
    )
```

```python
import functools
import math

import jax
import jax.numpy as jnp
from jax import lax
from jax.experimental import pallas as pl
from jax.experimental.pallas import tpu as pltpu
from jax.sharding import PartitionSpec as P

FIELD = 18
MAPS = 8
STRIDE = 2
TILE_PX = 16
INPUTS = 972
HALO = 16
POS = 64
SPAN = TILE_PX + HALO
SIDE_POS = TILE_PX // STRIDE
UNITS = POS * MAPS
HALF = UNITS // 2
PLANE = SPAN * SPAN
QUAD = TILE_PX * TILE_PX
PATCH = FIELD * FIELD
LANES = 128
PAD_IN = -(-INPUTS // LANES) * LANES
PAD_STRIP = -(-FIELD * SPAN // LANES) * LANES
GRAB = 512
STEP_IN = 256
LAST = INPUTS % LANES

sparsity_weight = 1.0
smooth_eps = 0.01
guard_eps = 1e-06

BF = jnp.bfloat16
F32 = jnp.float32
VMEM_CAP = 24 * 1024 * 1024
RELAY_TILES = 4


def send(value, axis, pairs):
    return lax.ppermute(value, axis, pairs)


def ring(count, steps):
    return [(s, (s + steps) % count) for s in range(count)]


def flips(count, flip):
    return [(s, s ^ flip) for s in range(count)]


def flip_all(pairs):
    return [(b, a) for a, b in pairs]


def routes(n_tile):
    side = math.isqrt(n_tile)
    if n_tile == RELAY_TILES:
        return (
            [(0, 2), (3, 1), (1, 0), (2, 3)],
            [(1, 3), (2, 0), (0, 1), (3, 2)],
            [(1, 2), (2, 1)],
            [(2, 3), (1, 0)],
        )
    return ring(n_tile, -1), ring(n_tile, -side), ring(n_tile, -side - 1), None


def quadrants():
    if lax.axis_size("tile") != RELAY_TILES:
        return 1, 2, 3
    t = lax.axis_index("tile")
    inner = (t == 1) | (t == 2)
    first = jnp.where(inner, 2, jnp.where(t == 0, 1, 3))
    second = jnp.where(t == 1, 3, jnp.where(t == 2, 1, 2))
    third = jnp.where(t % 2 == 0, 3, 1)
    return first, second, third


def kernel_call(body, outs, scratch=(), n_in=0, flops=0, name=None, scalar_out=False):
    places = [pltpu.VMEM] * (len(outs) - scalar_out) + [pltpu.SMEM] * scalar_out
    return pl.pallas_call(
        body,
        out_shape=outs,
        in_specs=[pl.BlockSpec(memory_space=pltpu.VMEM)] * n_in,
        out_specs=tuple(pl.BlockSpec(memory_space=place) for place in places),
        scratch_shapes=list(scratch),
        compiler_params=pltpu.CompilerParams(vmem_limit_bytes=VMEM_CAP),
        cost_estimate=pl.CostEstimate(flops=flops, transcendentals=0, bytes_accessed=flops // 256),
        name=name,
    )


def positions(rows):
    for i in range(rows):
        for j in range(0, SIDE_POS, 2):
            lead = i * STRIDE * SPAN // LANES * LANES
            rest = i * STRIDE * SPAN - lead
            yield (i * SIDE_POS + j) * MAPS, lead, (rest + STRIDE * j, rest + STRIDE * (j + 1))


def place(dst, own, slots):
    for q, load in zip((0,) + tuple(quadrants()), (own,) + tuple(slots)):
        top = pl.multiple_of(q // 2 * TILE_PX, TILE_PX)
        left = pl.multiple_of(q % 2 * TILE_PX, TILE_PX)
        for ch in range(3):
            dst[ch, pl.ds(top, TILE_PX), pl.ds(left, TILE_PX), :] = load(ch)


def loader(*refs):
    def load(ch):
        value = refs[0][ch]
        for ref in refs[1:]:
            value = value + ref[ch]
        return value

    return load


def expand_body(w_ref, con_ref, x_ref, wd_ref, wt_ref, st_ref, copy_ref, wp_ref, v_ref, s_ref):
    copy_ref[...] = x_ref[...]
    wp_ref[:, PAD_IN - LANES :] = jnp.zeros((UNITS, LANES), BF)
    wp_ref[:, :INPUTS] = w_ref[...]

    def wanted(shape, axis):
        n = lax.broadcasted_iota(jnp.int32, shape, axis)
        row, col = n // SPAN, n % SPAN
        return (col < FIELD) & (row < FIELD), row * FIELD + col

    inside, source = wanted((1, PAD_STRIP), 1)
    inside_t, source_t = wanted((PAD_STRIP, 1), 0)
    k = lax.broadcasted_iota(jnp.int32, (GRAB, PAD_STRIP), 0)
    k_t = lax.broadcasted_iota(jnp.int32, (PAD_STRIP, GRAB), 1)
    for ch in range(3):
        skip = ch * (PATCH - STEP_IN)
        want = jnp.where(inside, source + skip, -1)
        s_ref[...] = jnp.where(k == want, 1.0, 0.0).astype(BF)
        want = jnp.where(inside_t, source_t + skip, -1)
        st_ref[ch] = jnp.where(k_t == want, 1.0, 0.0).astype(BF)
        v = jnp.dot(
            wp_ref[:, ch * STEP_IN : ch * STEP_IN + GRAB], s_ref[...], preferred_element_type=F32
        )
        v_ref[...] = v * con_ref[:, ch : ch + 1]
        base = ch * PLANE
        for u, lead, shifts in positions(SIDE_POS):
            parts = []
            for h, s in enumerate(shifts):
                blk = v_ref[u + h * MAPS : u + (h + 1) * MAPS, :]
                parts.append(pltpu.roll(blk, s, 1) if s else blk)
            rows = slice(u, u + 2 * MAPS)
            if lead:
                wd_ref[rows, base : base + lead] = jnp.zeros((2 * MAPS, lead), BF)
            end = lead + PAD_STRIP
            wd_ref[rows, base + lead : base + end] = jnp.concatenate(parts, 0).astype(BF)
            if end < PLANE:
                wd_ref[rows, base + end : base + PLANE] = jnp.zeros((2 * MAPS, PLANE - end), BF)
        for at in range(0, PLANE, LANES):
            flipped = wd_ref[:, base + at : base + at + LANES].T
            for sub in range(0, LANES, TILE_PX):
                row, col = (at + sub) // SPAN, (at + sub) % SPAN
                q = row // TILE_PX * 2 + col // TILE_PX
                to = ch * QUAD + row % TILE_PX * TILE_PX
                wt_ref[q, to : to + TILE_PX, :] = flipped[sub : sub + TILE_PX]


def coded_body(relay, x_ref, *refs):
    slots, (wd_ref, wt_ref, coded_ref, out_ref, xe) = refs[: 4 if relay else 3], refs[-5:]
    third = slots[2:]
    place(xe, loader(x_ref), (loader(slots[0]), loader(slots[1]), loader(*third)))
    batch = x_ref.shape[-1]
    coded = jnp.dot(wd_ref[...], xe[...].reshape(3 * PLANE, batch), preferred_element_type=F32)
    coded_ref[...] = coded
    part = jnp.dot(wt_ref[quadrants()[2]], coded.astype(BF), preferred_element_type=F32)
    out_ref[...] = part.astype(BF).reshape(out_ref.shape)


def spill_body(wt_ref, coded_ref, a_ref, b_ref):
    rounded = coded_ref[...].astype(BF)
    first, second, _ = quadrants()
    for q, ref in ((second, b_ref), (first, a_ref)):
        part = jnp.dot(wt_ref[q], rounded, preferred_element_type=F32)
        ref[...] = part.astype(BF).reshape(ref.shape)


def own_body(wt_ref, coded_ref, x_ref, own_ref, loss_ref):
    coded = coded_ref[...]
    batch = coded.shape[-1]
    part = jnp.dot(wt_ref[0], coded.astype(BF), preferred_element_type=F32)
    own_ref[...] = part.reshape(own_ref.shape) - x_ref[...].astype(F32)
    root = jnp.sqrt(smooth_eps + coded * coded)
    loss_ref[...] = sparsity_weight * jnp.sum(root.reshape(UNITS // 8, 8, batch), 0)


def join_body(a_ref, d_ref, out_ref):
    out_ref[...] = (a_ref[...].astype(F32) + d_ref[...].astype(F32)).astype(BF)


def error_body(own, fa, fb, fc, sp, e_ref, loss_ref):
    batch = own.shape[-1]
    total = sp[...]
    for ch in range(3):
        err = own[ch] + fa[ch].astype(F32) + fb[ch].astype(F32) + fc[ch].astype(F32)
        e_ref[ch] = err.astype(BF)
        total = total + jnp.sum((err * err).reshape(QUAD // 8, 8, batch), 0)
    loss_ref[...] = total


def ready_body(relay, coded_ref, e_ref, x_ref, *refs):
    slots, (left_ref, pull_ref, xe, copy_ref) = refs[:-4], refs[-4:]
    copy_ref[...] = e_ref[...]
    coded = coded_ref[...]
    left_ref[...] = (2.0 * coded).astype(BF)
    pull_ref[...] = sparsity_weight * coded / jnp.sqrt(smooth_eps + coded * coded)
    place(xe, loader(x_ref), (loader(slots[0]), loader(slots[1]), loader(*slots[2:])))


def gradient_rows(half, wd_ref, left_ref, pull_ref, con_ref, st_ref, ex, gd, gs, out):
    at = pl.multiple_of(half * HALF, HALF)
    rows = pl.ds(at, HALF)
    batch = left_ref.shape[-1]
    e_all = ex[:, :, :batch].reshape(3 * PLANE, batch)
    enc = jnp.dot(wd_ref[rows, :], e_all, preferred_element_type=F32)
    left = left_ref[rows, :].astype(F32)
    right = 2.0 * enc + pull_ref[rows, :]
    con = con_ref[rows, :]
    shift = half * (SIDE_POS // 2 * STRIDE * SPAN)
    out[...] = jnp.zeros((HALF, PAD_IN), F32)
    for ch in range(3):
        opened = con[:, ch : ch + 1]
        both = jnp.concatenate([(left * opened).astype(BF), (right * opened).astype(BF)], 1)
        gd[...] = lax.dot_general(
            both, ex[ch], (((1,), (1,)), ((), ())), preferred_element_type=F32
        )
        for u, lead, shifts in positions(SIDE_POS // 2):
            parts = []
            lanes = pl.ds(pl.multiple_of(lead + shift, LANES), PAD_STRIP)
            for h, s in enumerate(shifts):
                blk = gd[u + h * MAPS : u + (h + 1) * MAPS, lanes]
                parts.append(pltpu.roll(blk, PAD_STRIP - s, 1) if s else blk)
            gs[u : u + 2 * MAPS, :] = jnp.concatenate(parts, 0).astype(BF)
        cols = slice(ch * STEP_IN, ch * STEP_IN + GRAB)
        out[:, cols] = out[:, cols] + jnp.dot(gs[...], st_ref[ch], preferred_element_type=F32)


def away_body(relay, wd_ref, left_ref, pull_ref, con_ref, st_ref, xe, e_ref, *refs):
    slots, (send_ref, ex, tmp, gd, gs, out) = refs[:-6], refs[-6:]
    batch = e_ref.shape[-1]
    place(tmp, loader(e_ref), (loader(slots[0]), loader(slots[1]), loader(*slots[2:])))
    for ch in range(3):
        ex[ch, :, :batch] = tmp[ch].reshape(PLANE, batch)
        ex[ch, :, batch:] = xe[ch].reshape(PLANE, batch)
    core = lax.axis_index("dp") % 2
    gradient_rows(1 - core, wd_ref, left_ref, pull_ref, con_ref, st_ref, ex, gd, gs, out)
    send_ref[...] = out[...].astype(BF)


def home_body(wd_ref, left_ref, pull_ref, con_ref, st_ref, ex, keep_ref, gd, gs):
    core = lax.axis_index("dp") % 2
    gradient_rows(core, wd_ref, left_ref, pull_ref, con_ref, st_ref, ex, gd, gs, keep_ref)


def pair_body(keep, got, *refs):
    own_ref, sends, scr = refs[0], refs[1:-1], refs[-1]
    rows = own_ref.shape[0]
    scr[...] = keep[...] + got[...].astype(F32)
    chip = lax.axis_index("dp") // 2
    own_ref[...] = scr[pl.ds(pl.multiple_of(chip * rows, rows), rows), :]
    for x, ref in enumerate(sends):
        at = pl.multiple_of((chip ^ (x + 1)) * rows, rows)
        ref[...] = scr[pl.ds(at, rows), :].astype(BF)


def pieces(value):
    high = value.astype(BF)
    rest = value - high.astype(F32)
    mid = rest.astype(BF)
    low = (rest - mid.astype(F32)).astype(BF)
    return high.astype(F32), mid.astype(F32), low.astype(F32)


def total_of(value):
    return jnp.sum(jnp.sum(value, 0, keepdims=True), 1, keepdims=True)


def shard_body(own, *refs):
    got, loss, shard_ref = refs[:-2], refs[-2], refs[-1]
    total = own[...]
    for ref in got:
        total = total + ref[...].astype(F32)
    lane = lax.broadcasted_iota(jnp.int32, (1, LANES), 1)
    tail = total[:, PAD_IN - LANES :]
    for at, value in enumerate(pieces(total_of(loss[...])) + pieces(total_of(total * total))):
        tail = jnp.where(lane == LAST + at, value, tail)
    shard_ref[:, : PAD_IN - LANES] = total[:, : PAD_IN - LANES].astype(BF)
    shard_ref[:, PAD_IN - LANES :] = tail.astype(BF)


def gather_body(own, *refs):
    got, half_ref = refs[:-1], refs[-1]
    rows = own.shape[0]
    chip = lax.axis_index("dp") // 2
    half_ref[pl.ds(pl.multiple_of(chip * rows, rows), rows), :] = own[...]
    for x, ref in enumerate(got):
        at = pl.multiple_of((chip ^ (x + 1)) * rows, rows)
        half_ref[pl.ds(at, rows), :] = ref[...]


def tally_body(rows, mine, other, tally_ref):
    total = jnp.zeros((8, LANES), F32)
    for ref in (mine, other):
        for at in range(0, HALF, rows):
            total = total + ref[at : at + TILE_PX, PAD_IN - LANES :].astype(F32)[:8]
    tally_ref[...] = total


def finish_body(entries, frames_total, mine, other, *refs):
    tallies, up_ref, loss_ref = refs[:-2], refs[-2], refs[-1]
    tally = tallies[0][...]
    for ref in tallies[1:]:
        tally = tally + ref[...]
    lane = lax.broadcasted_iota(jnp.int32, (1, LANES), 1)
    row = tally[:1]
    square = total_of(jnp.where((lane >= LAST + 3) & (lane < LAST + 6), row, 0.0))
    factor = -lax.rsqrt(square / entries + guard_eps)
    core = lax.axis_index("dp") % 2
    for half, ref in ((core, mine), (1 - core, other)):
        at = pl.multiple_of(half * HALF, HALF)
        up_ref[pl.ds(at, HALF), :] = (ref[:, :INPUTS].astype(F32) * factor).astype(BF)
    loss_ref[0, 0] = jnp.sum(jnp.where((lane >= LAST) & (lane < LAST + 3), row, 0.0)) / frames_total


def local(frames, weights, connect):
    batch = frames.shape[-1]
    n_tile = lax.axis_size("tile")
    n_dp = lax.axis_size("dp")
    chips = n_dp // 2
    sds = jax.ShapeDtypeStruct
    mac = 2 * UNITS * 3 * PLANE * batch
    quad = (3, TILE_PX, TILE_PX, batch)
    units = (UNITS, batch)
    plane = (3, SPAN, SPAN, batch)
    to_first, to_second, to_third, onward = routes(n_tile)
    relay = onward is not None

    def spread_out(now, later):
        first = send(now, "tile", to_first)
        second = send(later, "tile", to_second)
        third = send(later, "tile", to_third)
        return [first, second, third] + ([send(first, "tile", onward)] if relay else [])

    x0 = frames[0]
    con = connect.reshape(UNITS, 3).astype(F32)
    wd, wt, st, x_late = kernel_call(
        expand_body,
        (
            sds((UNITS, 3 * PLANE), BF),
            sds((4, 3 * QUAD, UNITS), BF),
            sds((3, PAD_STRIP, GRAB), BF),
            sds(quad, BF),
        ),
        [
            pltpu.VMEM((UNITS, PAD_IN), BF),
            pltpu.VMEM((UNITS, PAD_STRIP), F32),
            pltpu.VMEM((GRAB, PAD_STRIP), BF),
        ],
        n_in=3, flops=4 * mac, name="expand",
    )(weights.reshape(UNITS, INPUTS), con, x0)
    xs = spread_out(x0, x_late if relay else x0)

    coded, sc = kernel_call(
        functools.partial(coded_body, relay),
        (sds(units, F32), sds(quad, BF)),
        [pltpu.VMEM(plane, BF)],
        n_in=3 + len(xs), flops=mac, name="coded",
    )(x0, *xs, wd, wt)
    sa, sb = kernel_call(
        spill_body, (sds(quad, BF), sds(quad, BF)), n_in=2, flops=mac // 2, name="spill"
    )(wt, coded)
    if relay:
        passed = send(sc, "tile", flip_all(onward))
    fb = send(sb, "tile", flip_all(to_second))
    fc = send(sc, "tile", flip_all(to_third))
    own, sparse = kernel_call(
        own_body, (sds(quad, F32), sds((8, batch), F32)), n_in=3, flops=mac // 4, name="own"
    )(wt, coded, x0)
    if relay:
        (sa,) = kernel_call(join_body, (sds(quad, BF),), n_in=2, flops=mac // 64, name="join")(sa, passed)
    fa = send(sa, "tile", flip_all(to_first))
    e0, loss_part = kernel_call(
        error_body, (sds(quad, BF), sds((8, batch), F32)), n_in=5, flops=mac // 32, name="errors"
    )(own, fa, fb, fc, sparse)

    left, pull, xe, e_late = kernel_call(
        functools.partial(ready_body, relay),
        (sds(units, BF), sds(units, F32), sds(plane, BF), sds(quad, BF)),
        n_in=3 + len(xs), flops=mac // 16, name="ready",
    )(coded, e0, x0, *xs)
    es = spread_out(e0, e_late if relay else e0)

    half = (HALF, PAD_IN)
    work = [pltpu.VMEM((HALF, PLANE), F32), pltpu.VMEM((HALF, PAD_STRIP), BF)]
    away, ex = kernel_call(
        functools.partial(away_body, relay),
        (sds(half, BF), sds((3, PLANE, 2 * batch), BF)),
        [pltpu.VMEM(plane, BF)] + work + [pltpu.VMEM(half, F32)],
        n_in=7 + len(es), flops=2 * mac, name="away",
    )(wd, left, pull, con, st, xe, e0, *es)
    got = send(away, "dp", flips(n_dp, 1))
    (keep,) = kernel_call(
        home_body, (sds(half, F32),), work, n_in=6, flops=2 * mac, name="home"
    )(wd, left, pull, con, st, ex)

    rows = HALF // chips
    shard = sds((rows, PAD_IN), BF)
    split = kernel_call(
        pair_body,
        (sds((rows, PAD_IN), F32),) + (shard,) * (chips - 1),
        [pltpu.VMEM(half, F32)],
        n_in=2, flops=mac // 32, name="pair",
    )(keep, got)
    arrived = [send(v, "dp", flips(n_dp, 2 * (x + 1))) for x, v in enumerate(split[1:])]
    (mine,) = kernel_call(shard_body, (shard,), n_in=chips + 1, flops=mac // 64, name="shard")(
        split[0], *arrived, loss_part
    )
    others = [send(mine, "dp", flips(n_dp, 2 * x)) for x in range(1, chips)]
    (mine_half,) = kernel_call(gather_body, (sds(half, BF),), n_in=chips, flops=mac // 64, name="gather")(
        mine, *others
    )
    other_half = send(mine_half, "dp", flips(n_dp, 1))
    (tally,) = kernel_call(
        functools.partial(tally_body, rows), (sds((8, LANES), F32),), n_in=2, flops=mac // 64, name="tally"
    )(mine_half, other_half)
    tallies = [send(tally, "tile", ring(n_tile, s)) for s in range(1, n_tile)]

    entries = n_tile * POS * MAPS * INPUTS
    update, loss = kernel_call(
        functools.partial(finish_body, float(entries), float(batch * n_dp)),
        (sds((UNITS, INPUTS), BF), sds((1, 1), F32)),
        n_in=2 + n_tile, flops=mac // 32, name="finish", scalar_out=True,
    )(mine_half, other_half, tally, *tallies)
    return update.reshape(1, POS, MAPS, INPUTS), loss.reshape(())


def solution(mesh):
    placed = (
        P("tile", None, None, None, "dp"),
        P("tile", None, None, None),
        P("tile", None, None, None),
    )
    return jax.shard_map(
        local,
        mesh=mesh,
        in_specs=placed,
        out_specs=(P("tile", None, None, None), P()),
        check_vma=False,
    )
```

```python
import functools
import math

import jax
import jax.numpy as jnp
from jax import lax
from jax.experimental import pallas as pl
from jax.experimental.pallas import tpu as pltpu
from jax.sharding import PartitionSpec as P


FIELD = 18
MAPS = 8
STRIDE = 2
TILE_PX = 16
INPUTS = 972
HALO = 16
POS = 64
SPAN = TILE_PX + HALO
SIDE_POS = TILE_PX // STRIDE
UNITS = POS * MAPS
HALF = UNITS // 2
PLANE = SPAN * SPAN
QUAD = TILE_PX * TILE_PX
PATCH = FIELD * FIELD
LANES = 128
PAD_IN = -(-INPUTS // LANES) * LANES
PAD_STRIP = -(-FIELD * SPAN // LANES) * LANES
GRAB = 512
STEP_IN = 256
LAST = INPUTS % LANES

sparsity_weight = 1.0
smooth_eps = 0.01
guard_eps = 1e-06

BF = jnp.bfloat16
F32 = jnp.float32
VMEM_CAP = 24 * 1024 * 1024
RELAY_TILES = 4


def send(value, axis, pairs):
    return lax.ppermute(value, axis, pairs)


def ring(count, steps):
    return [(s, (s + steps) % count) for s in range(count)]


def flips(count, flip):
    return [(s, s ^ flip) for s in range(count)]


def flip_all(pairs):
    return [(b, a) for a, b in pairs]


def routes(n_tile):
    side = math.isqrt(n_tile)
    if n_tile == RELAY_TILES:
        return (
            [(0, 2), (3, 1), (1, 0), (2, 3)],
            [(1, 3), (2, 0), (0, 1), (3, 2)],
            [(1, 2), (2, 1), (0, 0), (3, 3)],
            [(2, 3), (1, 0), (0, 1), (3, 2)],
        )
    return ring(n_tile, -1), ring(n_tile, -side), ring(n_tile, -side - 1), None


def inner_tile():
    t = lax.axis_index("tile")
    return (t == 1) | (t == 2)


def quadrants():
    if lax.axis_size("tile") != RELAY_TILES:
        return 1, 2, 3
    t = lax.axis_index("tile")
    first = jnp.where(inner_tile(), 2, jnp.where(t == 0, 1, 3))
    second = jnp.where(t == 1, 3, jnp.where(t == 2, 1, 2))
    third = jnp.where(t % 2 == 0, 3, 1)
    return first, second, third


def spilled():
    return quadrants()[::-1]


def kernel_call(body, outs, scratch=(), n_in=0, flops=0, scalar_out=False):
    places = [pltpu.VMEM] * (len(outs) - scalar_out) + [pltpu.SMEM] * scalar_out
    return pl.pallas_call(
        body,
        out_shape=outs,
        in_specs=[pl.BlockSpec(memory_space=pltpu.VMEM)] * n_in,
        out_specs=tuple(pl.BlockSpec(memory_space=place) for place in places),
        scratch_shapes=list(scratch),
        compiler_params=pltpu.CompilerParams(vmem_limit_bytes=VMEM_CAP),
        cost_estimate=pl.CostEstimate(flops=flops, transcendentals=0, bytes_accessed=flops // 256),
    )


def positions(rows):
    for i in range(rows):
        for j in range(0, SIDE_POS, 2):
            lead = i * STRIDE * SPAN // LANES * LANES
            rest = i * STRIDE * SPAN - lead
            yield (i * SIDE_POS + j) * MAPS, lead, (rest + STRIDE * j, rest + STRIDE * (j + 1))


def place(dst, own, slots):
    def put(q, ref):
        top = pl.multiple_of(q // 2 * TILE_PX, TILE_PX)
        left = pl.multiple_of(q % 2 * TILE_PX, TILE_PX)
        for ch in range(3):
            dst[ch, pl.ds(top, TILE_PX), pl.ds(left, TILE_PX), :] = ref[ch]

    first, second, third = quadrants()
    put(0, own)
    put(first, slots[0])
    put(second, slots[1])
    if len(slots) == 3:
        put(third, slots[2])
    else:
        inner = inner_tile()
        pl.when(inner)(lambda: put(third, slots[2]))
        pl.when(jnp.logical_not(inner))(lambda: put(third, slots[3]))


def stage_body(w_ref, x_ref, wp_ref, copy_ref):
    copy_ref[...] = x_ref[...]
    wp_ref[:, PAD_IN - LANES :] = jnp.zeros((UNITS, LANES), BF)
    wp_ref[:, :INPUTS] = w_ref[...]


def expand_body(wp_ref, con_ref, wd_ref, wt_ref, st_ref, v_ref, s_ref):
    def wanted(shape, axis):
        n = lax.broadcasted_iota(jnp.int32, shape, axis)
        row, col = n // SPAN, n % SPAN
        return (col < FIELD) & (row < FIELD), row * FIELD + col

    inside, source = wanted((1, PAD_STRIP), 1)
    inside_t, source_t = wanted((PAD_STRIP, 1), 0)
    k = lax.broadcasted_iota(jnp.int32, (GRAB, PAD_STRIP), 0)
    k_t = lax.broadcasted_iota(jnp.int32, (PAD_STRIP, GRAB), 1)
    for ch in range(3):
        skip = ch * (PATCH - STEP_IN)
        want = jnp.where(inside, source + skip, -1)
        s_ref[...] = jnp.where(k == want, 1.0, 0.0).astype(BF)
        want = jnp.where(inside_t, source_t + skip, -1)
        st_ref[ch] = jnp.where(k_t == want, 1.0, 0.0).astype(BF)
        v = jnp.dot(
            wp_ref[:, ch * STEP_IN : ch * STEP_IN + GRAB], s_ref[...], preferred_element_type=F32
        )
        v_ref[...] = v * con_ref[:, ch : ch + 1]
        base = ch * PLANE
        for u, lead, shifts in positions(SIDE_POS):
            parts = []
            for h, s in enumerate(shifts):
                blk = v_ref[u + h * MAPS : u + (h + 1) * MAPS, :]
                parts.append(pltpu.roll(blk, s, 1) if s else blk)
            rows = slice(u, u + 2 * MAPS)
            if lead:
                wd_ref[rows, base : base + lead] = jnp.zeros((2 * MAPS, lead), BF)
            end = lead + PAD_STRIP
            wd_ref[rows, base + lead : base + end] = jnp.concatenate(parts, 0).astype(BF)
            if end < PLANE:
                wd_ref[rows, base + end : base + PLANE] = jnp.zeros((2 * MAPS, PLANE - end), BF)
        for at in range(0, PLANE, LANES):
            flipped = wd_ref[:, base + at : base + at + LANES].T
            for sub in range(0, LANES, TILE_PX):
                row, col = (at + sub) // SPAN, (at + sub) % SPAN
                q = row // TILE_PX * 2 + col // TILE_PX
                to = ch * QUAD + row % TILE_PX * TILE_PX
                wt_ref[q, to : to + TILE_PX, :] = flipped[sub : sub + TILE_PX]


def decoded(wt_ref, q, rounded, shape):
    return jnp.dot(wt_ref[q], rounded, preferred_element_type=F32).reshape(shape)


def coded_body(x_ref, *refs):
    slots, (wd_ref, wt_ref, coded_ref, out_ref, xe) = refs[:-5], refs[-5:]
    place(xe, x_ref, slots)
    batch = x_ref.shape[-1]
    coded = jnp.dot(wd_ref[...], xe[...].reshape(3 * PLANE, batch), preferred_element_type=F32)
    coded_ref[...] = coded
    out_ref[...] = decoded(wt_ref, spilled()[0], coded.astype(BF), out_ref.shape).astype(BF)


def spill_body(wt_ref, coded_ref, *outs):
    rounded = coded_ref[...].astype(BF)
    for q, ref in zip(spilled()[1:], outs):
        ref[...] = decoded(wt_ref, q, rounded, ref.shape).astype(BF)


def own_body(wt_ref, coded_ref, x_ref, own_ref, loss_ref, *last):
    coded = coded_ref[...]
    rounded = coded.astype(BF)
    batch = coded.shape[-1]
    for ref in last:
        ref[...] = decoded(wt_ref, spilled()[2], rounded, ref.shape)
    own_ref[...] = decoded(wt_ref, 0, rounded, own_ref.shape) - x_ref[...].astype(F32)
    root = jnp.sqrt(smooth_eps + coded * coded)
    loss_ref[...] = sparsity_weight * jnp.sum(root.reshape(UNITS // 8, 8, batch), 0)


def join_body(last, passed, out_ref):
    out_ref[...] = (last[...] + passed[...].astype(F32)).astype(BF)


def error_body(own, sp, *refs):
    parts, (e_ref, loss_ref) = refs[:-2], refs[-2:]
    batch = own.shape[-1]
    total = sp[...]
    for ch in range(3):
        err = own[ch]
        for ref in parts:
            err = err + ref[ch].astype(F32)
        e_ref[ch] = err.astype(BF)
        total = total + jnp.sum((err * err).reshape(QUAD // 8, 8, batch), 0)
    loss_ref[...] = total


def ready_body(coded_ref, e_ref, x_ref, *refs):
    slots, (left_ref, pull_ref, xe, copy_ref) = refs[:-4], refs[-4:]
    copy_ref[...] = e_ref[...]
    coded = coded_ref[...]
    left_ref[...] = (2.0 * coded).astype(BF)
    pull_ref[...] = sparsity_weight * coded / jnp.sqrt(smooth_eps + coded * coded)
    place(xe, x_ref, slots)


def gradient_rows(half, wd_ref, left_ref, pull_ref, con_ref, st_ref, ex, gd, gs, out):
    at = pl.multiple_of(half * HALF, HALF)
    rows = pl.ds(at, HALF)
    batch = left_ref.shape[-1]
    e_all = ex[:, :, :batch].reshape(3 * PLANE, batch)
    enc = jnp.dot(wd_ref[rows, :], e_all, preferred_element_type=F32)
    left = left_ref[rows, :].astype(F32)
    right = 2.0 * enc + pull_ref[rows, :]
    con = con_ref[rows, :]
    shift = half * (SIDE_POS // 2 * STRIDE * SPAN)
    out[...] = jnp.zeros((HALF, PAD_IN), F32)
    for ch in range(3):
        opened = con[:, ch : ch + 1]
        both = jnp.concatenate([(left * opened).astype(BF), (right * opened).astype(BF)], 1)
        gd[...] = lax.dot_general(
            both, ex[ch], (((1,), (1,)), ((), ())), preferred_element_type=F32
        )
        for u, lead, shifts in positions(SIDE_POS // 2):
            parts = []
            lanes = pl.ds(pl.multiple_of(lead + shift, LANES), PAD_STRIP)
            for h, s in enumerate(shifts):
                blk = gd[u + h * MAPS : u + (h + 1) * MAPS, lanes]
                parts.append(pltpu.roll(blk, PAD_STRIP - s, 1) if s else blk)
            gs[u : u + 2 * MAPS, :] = jnp.concatenate(parts, 0).astype(BF)
        cols = slice(ch * STEP_IN, ch * STEP_IN + GRAB)
        out[:, cols] = out[:, cols] + jnp.dot(gs[...], st_ref[ch], preferred_element_type=F32)


def away_body(wd_ref, left_ref, pull_ref, con_ref, st_ref, xe, e_ref, *refs):
    slots, (send_ref, ex, tmp, gd, gs, out) = refs[:-6], refs[-6:]
    batch = e_ref.shape[-1]
    place(tmp, e_ref, slots)
    for ch in range(3):
        ex[ch, :, :batch] = tmp[ch].reshape(PLANE, batch)
        ex[ch, :, batch:] = xe[ch].reshape(PLANE, batch)
    core = lax.axis_index("dp") % 2
    gradient_rows(1 - core, wd_ref, left_ref, pull_ref, con_ref, st_ref, ex, gd, gs, out)
    send_ref[...] = out[...].astype(BF)


def home_body(wd_ref, left_ref, pull_ref, con_ref, st_ref, ex, keep_ref, gd, gs):
    core = lax.axis_index("dp") % 2
    gradient_rows(core, wd_ref, left_ref, pull_ref, con_ref, st_ref, ex, gd, gs, keep_ref)


def pair_body(keep, got, *refs):
    own_ref, sends, scr = refs[0], refs[1:-1], refs[-1]
    rows = own_ref.shape[0]
    scr[...] = keep[...] + got[...].astype(F32)
    chip = lax.axis_index("dp") // 2
    own_ref[...] = scr[pl.ds(pl.multiple_of(chip * rows, rows), rows), :]
    for x, ref in enumerate(sends):
        at = pl.multiple_of((chip ^ (x + 1)) * rows, rows)
        ref[...] = scr[pl.ds(at, rows), :].astype(BF)


def pieces(value):
    high = value.astype(BF)
    rest = value - high.astype(F32)
    mid = rest.astype(BF)
    low = (rest - mid.astype(F32)).astype(BF)
    return high.astype(F32), mid.astype(F32), low.astype(F32)


def total_of(value):
    return jnp.sum(jnp.sum(value, 0, keepdims=True), 1, keepdims=True)


def shard_body(own, *refs):
    got, loss, shard_ref = refs[:-2], refs[-2], refs[-1]
    total = own[...]
    for ref in got:
        total = total + ref[...].astype(F32)
    lane = lax.broadcasted_iota(jnp.int32, (1, LANES), 1)
    tail = total[:, PAD_IN - LANES :]
    for at, value in enumerate(pieces(total_of(loss[...])) + pieces(total_of(total * total))):
        tail = jnp.where(lane == LAST + at, value, tail)
    shard_ref[:, : PAD_IN - LANES] = total[:, : PAD_IN - LANES].astype(BF)
    shard_ref[:, PAD_IN - LANES :] = tail.astype(BF)


def gather_body(own, *refs):
    got, half_ref = refs[:-1], refs[-1]
    rows = own.shape[0]
    chip = lax.axis_index("dp") // 2
    half_ref[pl.ds(pl.multiple_of(chip * rows, rows), rows), :] = own[...]
    for x, ref in enumerate(got):
        at = pl.multiple_of((chip ^ (x + 1)) * rows, rows)
        half_ref[pl.ds(at, rows), :] = ref[...]


def tally_body(rows, mine, other, tally_ref):
    total = jnp.zeros((8, LANES), F32)
    for ref in (mine, other):
        for at in range(0, HALF, rows):
            total = total + ref[at : at + TILE_PX, PAD_IN - LANES :].astype(F32)[:8]
    tally_ref[...] = total


def finish_body(entries, frames_total, mine, other, *refs):
    tallies, up_ref, loss_ref = refs[:-2], refs[-2], refs[-1]
    tally = tallies[0][...]
    for ref in tallies[1:]:
        tally = tally + ref[...]
    lane = lax.broadcasted_iota(jnp.int32, (1, LANES), 1)
    row = tally[:1]
    square = total_of(jnp.where((lane >= LAST + 3) & (lane < LAST + 6), row, 0.0))
    factor = -lax.rsqrt(square / entries + guard_eps)
    core = lax.axis_index("dp") % 2
    for half, ref in ((core, mine), (1 - core, other)):
        at = pl.multiple_of(half * HALF, HALF)
        up_ref[pl.ds(at, HALF), :] = (ref[:, :INPUTS].astype(F32) * factor).astype(BF)
    loss_ref[0, 0] = jnp.sum(jnp.where((lane >= LAST) & (lane < LAST + 3), row, 0.0)) / frames_total


def local(frames, weights, connect):
    batch = frames.shape[-1]
    n_tile = lax.axis_size("tile")
    n_dp = lax.axis_size("dp")
    chips = n_dp // 2
    sds = jax.ShapeDtypeStruct
    mac = 2 * UNITS * 3 * PLANE * batch
    quad = (3, TILE_PX, TILE_PX, batch)
    units = (UNITS, batch)
    plane = (3, SPAN, SPAN, batch)
    to_first, to_second, to_third, onward = routes(n_tile)
    relay = onward is not None

    def spread_out(now, later):
        first = send(now, "tile", to_first)
        second = send(later, "tile", to_second)
        third = send(later, "tile", to_third)
        if not relay:
            return [first, second, third]
        return [first, second, third, send(first, "tile", onward)]

    x0 = frames[0]
    con = connect.reshape(UNITS, 3).astype(F32)
    wp, x_late = kernel_call(
        stage_body, (sds((UNITS, PAD_IN), BF), sds(quad, BF)), n_in=2, flops=mac // 64
    )(weights.reshape(UNITS, INPUTS), x0)
    xs = spread_out(x0, x_late if relay else x0)
    wd, wt, st = kernel_call(
        expand_body,
        (sds((UNITS, 3 * PLANE), BF), sds((4, 3 * QUAD, UNITS), BF), sds((3, PAD_STRIP, GRAB), BF)),
        [pltpu.VMEM((UNITS, PAD_STRIP), F32), pltpu.VMEM((GRAB, PAD_STRIP), BF)],
        n_in=2, flops=4 * mac,
    )(wp, con)

    coded, s1 = kernel_call(
        coded_body,
        (sds(units, F32), sds(quad, BF)),
        [pltpu.VMEM(plane, BF)],
        n_in=3 + len(xs), flops=mac,
    )(x0, *xs, wd, wt)
    parts = []
    if relay:
        passed = send(s1, "tile", [(0, 1), (3, 2)])
    parts.append(send(s1, "tile", [(1, 2), (2, 1)] if relay else flip_all(to_third)))
    s2, *s3 = kernel_call(
        spill_body,
        (sds(quad, BF),) * (1 if relay else 2),
        n_in=2, flops=mac // 4,
    )(wt, coded)
    parts.append(send(s2, "tile", flip_all(to_second)))
    own, sparse, *last = kernel_call(
        own_body,
        (sds(quad, F32), sds((8, batch), F32)) + (sds(quad, F32),) * relay,
        n_in=3, flops=mac // 2,
    )(wt, coded, x0)
    if relay:
        s3 = kernel_call(join_body, (sds(quad, BF),), n_in=2, flops=mac // 64)(last[0], passed)
    parts.append(send(s3[0], "tile", flip_all(to_first)))
    e0, loss_part = kernel_call(
        error_body, (sds(quad, BF), sds((8, batch), F32)), n_in=2 + len(parts), flops=mac // 32
    )(own, sparse, *parts)

    left, pull, xe, e_late = kernel_call(
        ready_body,
        (sds(units, BF), sds(units, F32), sds(plane, BF), sds(quad, BF)),
        n_in=3 + len(xs), flops=mac // 16,
    )(coded, e0, x0, *xs)
    es = spread_out(e0, e_late if relay else e0)

    half = (HALF, PAD_IN)
    work = [pltpu.VMEM((HALF, PLANE), F32), pltpu.VMEM((HALF, PAD_STRIP), BF)]
    away, ex = kernel_call(
        away_body,
        (sds(half, BF), sds((3, PLANE, 2 * batch), BF)),
        [pltpu.VMEM(plane, BF)] + work + [pltpu.VMEM(half, F32)],
        n_in=7 + len(es), flops=2 * mac,
    )(wd, left, pull, con, st, xe, e0, *es)
    got = send(away, "dp", flips(n_dp, 1))
    (keep,) = kernel_call(
        home_body, (sds(half, F32),), work, n_in=6, flops=2 * mac
    )(wd, left, pull, con, st, ex)

    rows = HALF // chips
    shard = sds((rows, PAD_IN), BF)
    split = kernel_call(
        pair_body,
        (sds((rows, PAD_IN), F32),) + (shard,) * (chips - 1),
        [pltpu.VMEM(half, F32)],
        n_in=2, flops=mac // 32,
    )(keep, got)
    arrived = [send(v, "dp", flips(n_dp, 2 * (x + 1))) for x, v in enumerate(split[1:])]
    (mine,) = kernel_call(shard_body, (shard,), n_in=chips + 1, flops=mac // 64)(
        split[0], *arrived, loss_part
    )
    others = [send(mine, "dp", flips(n_dp, 2 * x)) for x in range(1, chips)]
    (mine_half,) = kernel_call(gather_body, (sds(half, BF),), n_in=chips, flops=mac // 64)(
        mine, *others
    )
    other_half = send(mine_half, "dp", flips(n_dp, 1))
    (tally,) = kernel_call(
        functools.partial(tally_body, rows), (sds((8, LANES), F32),), n_in=2, flops=mac // 64
    )(mine_half, other_half)
    tallies = [send(tally, "tile", ring(n_tile, s)) for s in range(1, n_tile)]

    entries = n_tile * POS * MAPS * INPUTS
    update, loss = kernel_call(
        functools.partial(finish_body, float(entries), float(batch * n_dp)),
        (sds((UNITS, INPUTS), BF), sds((1, 1), F32)),
        n_in=2 + n_tile, flops=mac // 32, scalar_out=True,
    )(mine_half, other_half, tally, *tallies)
    return update.reshape(1, POS, MAPS, INPUTS), loss.reshape(())


def solution(mesh):
    placed = (
        P("tile", None, None, None, "dp"),
        P("tile", None, None, None),
        P("tile", None, None, None),
    )
    return jax.shard_map(
        local,
        mesh=mesh,
        in_specs=placed,
        out_specs=(P("tile", None, None, None), P()),
        check_vma=False,
    )
```

```python
import functools
import math

import jax
import jax.numpy as jnp
from jax import lax
from jax.experimental import pallas as pl
from jax.experimental.pallas import tpu as pltpu
from jax.sharding import PartitionSpec as P


FIELD = 18
MAPS = 8
STRIDE = 2
TILE_PX = 16
INPUTS = 972
HALO = 16
POS = 64
SPAN = TILE_PX + HALO
SIDE_POS = TILE_PX // STRIDE
UNITS = POS * MAPS
HALF = UNITS // 2
PLANE = SPAN * SPAN
QUAD = TILE_PX * TILE_PX
PATCH = FIELD * FIELD
LANES = 128
PAD_IN = -(-INPUTS // LANES) * LANES
PAD_STRIP = -(-FIELD * SPAN // LANES) * LANES
GRAB = 512
STEP_IN = 256

sparsity_weight = 1.0
smooth_eps = 0.01
guard_eps = 1e-06


BF = jnp.bfloat16
F32 = jnp.float32
VMEM_CAP = 24 * 1024 * 1024
RELAY_TILES = 4


def send(value, axis, pairs):
    return lax.ppermute(value, axis, pairs)


def ring(count, steps):
    return [(s, (s + steps) % count) for s in range(count)]


def flips(count, flip):
    return [(s, s ^ flip) for s in range(count)]


def in_turn(values, axis, routes):
    out = []
    for value, pairs in zip(values, routes):
        out.append(send(value, axis, pairs))
    return out


def flip_all(pairs):
    return [(b, a) for a, b in pairs]


def routes(n_tile):
    side = math.isqrt(n_tile)
    if n_tile == RELAY_TILES:
        return (
            [(0, 2), (3, 1), (1, 0), (2, 3)],
            [(1, 3), (2, 0), (0, 1), (3, 2)],
            [(1, 2), (2, 1), (0, 0), (3, 3)],
            [(2, 3), (1, 0), (0, 1), (3, 2)],
        )
    return ring(n_tile, -1), ring(n_tile, -side), ring(n_tile, -side - 1), None


def inner_tile():
    t = lax.axis_index("tile")
    return (t == 1) | (t == 2)


def quadrants():
    if lax.axis_size("tile") != RELAY_TILES:
        return 1, 2, 3
    t = lax.axis_index("tile")
    first = jnp.where(inner_tile(), 2, jnp.where(t == 0, 1, 3))
    second = jnp.where(t == 1, 3, jnp.where(t == 2, 1, 2))
    third = jnp.where(t % 2 == 0, 3, 1)
    return first, second, third


def spilled():
    return quadrants()[::-1]


def kernel_call(body, outs, scratch=(), n_in=0, flops=0, scalar_out=False):
    places = [pltpu.VMEM] * (len(outs) - scalar_out) + [pltpu.SMEM] * scalar_out
    return pl.pallas_call(
        body,
        out_shape=outs,
        in_specs=[pl.BlockSpec(memory_space=pltpu.VMEM)] * n_in,
        out_specs=tuple(pl.BlockSpec(memory_space=place) for place in places),
        scratch_shapes=list(scratch),
        compiler_params=pltpu.CompilerParams(vmem_limit_bytes=VMEM_CAP),
        cost_estimate=pl.CostEstimate(flops=flops, transcendentals=0, bytes_accessed=flops // 256),
    )


def positions(rows):
    for i in range(rows):
        for j in range(0, SIDE_POS, 2):
            lead = i * STRIDE * SPAN // LANES * LANES
            rest = i * STRIDE * SPAN - lead
            yield (i * SIDE_POS + j) * MAPS, lead, (rest + STRIDE * j, rest + STRIDE * (j + 1))


def place(dst, own, slots):
    def put(q, ref):
        top = pl.multiple_of(q // 2 * TILE_PX, TILE_PX)
        left = pl.multiple_of(q % 2 * TILE_PX, TILE_PX)
        for ch in range(3):
            dst[ch, pl.ds(top, TILE_PX), pl.ds(left, TILE_PX), :] = ref[ch]

    first, second, third = quadrants()
    put(0, own)
    put(first, slots[0])
    put(second, slots[1])
    if len(slots) == 3:
        put(third, slots[2])
    else:
        inner = inner_tile()
        pl.when(inner)(lambda: put(third, slots[2]))
        pl.when(jnp.logical_not(inner))(lambda: put(third, slots[3]))


def stage_body(w_ref, x_ref, wp_ref, copy_ref):
    copy_ref[...] = x_ref[...]
    wp_ref[:, PAD_IN - LANES :] = jnp.zeros((UNITS, LANES), BF)
    wp_ref[:, :INPUTS] = w_ref[...]


def expand_body(wp_ref, con_ref, wd_ref, wt_ref, st_ref, v_ref, s_ref):
    def wanted(shape, axis):
        n = lax.broadcasted_iota(jnp.int32, shape, axis)
        row, col = n // SPAN, n % SPAN
        return (col < FIELD) & (row < FIELD), row * FIELD + col

    inside, source = wanted((1, PAD_STRIP), 1)
    inside_t, source_t = wanted((PAD_STRIP, 1), 0)
    k = lax.broadcasted_iota(jnp.int32, (GRAB, PAD_STRIP), 0)
    k_t = lax.broadcasted_iota(jnp.int32, (PAD_STRIP, GRAB), 1)
    for ch in range(3):
        skip = ch * (PATCH - STEP_IN)
        want = jnp.where(inside, source + skip, -1)
        s_ref[...] = jnp.where(k == want, 1.0, 0.0).astype(BF)
        want = jnp.where(inside_t, source_t + skip, -1)
        st_ref[ch] = jnp.where(k_t == want, 1.0, 0.0).astype(BF)
        v = jnp.dot(
            wp_ref[:, ch * STEP_IN : ch * STEP_IN + GRAB], s_ref[...], preferred_element_type=F32
        )
        v_ref[...] = v * con_ref[:, ch : ch + 1]
        base = ch * PLANE
        for u, lead, shifts in positions(SIDE_POS):
            parts = []
            for h, s in enumerate(shifts):
                blk = v_ref[u + h * MAPS : u + (h + 1) * MAPS, :]
                parts.append(pltpu.roll(blk, s, 1) if s else blk)
            rows = slice(u, u + 2 * MAPS)
            if lead:
                wd_ref[rows, base : base + lead] = jnp.zeros((2 * MAPS, lead), BF)
            end = lead + PAD_STRIP
            wd_ref[rows, base + lead : base + end] = jnp.concatenate(parts, 0).astype(BF)
            if end < PLANE:
                wd_ref[rows, base + end : base + PLANE] = jnp.zeros((2 * MAPS, PLANE - end), BF)
        for at in range(0, PLANE, LANES):
            flipped = wd_ref[:, base + at : base + at + LANES].T
            for sub in range(0, LANES, TILE_PX):
                row, col = (at + sub) // SPAN, (at + sub) % SPAN
                q = row // TILE_PX * 2 + col // TILE_PX
                to = ch * QUAD + row % TILE_PX * TILE_PX
                wt_ref[q, to : to + TILE_PX, :] = flipped[sub : sub + TILE_PX]


def decoded(wt_ref, q, rounded, shape):
    return jnp.dot(wt_ref[q], rounded, preferred_element_type=F32).reshape(shape)


def coded_body(x_ref, *refs):
    slots, (wd_ref, wt_ref, coded_ref, out_ref, xe) = refs[:-5], refs[-5:]
    place(xe, x_ref, slots)
    batch = x_ref.shape[-1]
    coded = jnp.dot(wd_ref[...], xe[...].reshape(3 * PLANE, batch), preferred_element_type=F32)
    coded_ref[...] = coded
    out_ref[...] = decoded(wt_ref, spilled()[0], coded.astype(BF), out_ref.shape).astype(BF)


def spill_body(wt_ref, coded_ref, *outs):
    rounded = coded_ref[...].astype(BF)
    for q, ref in zip(spilled()[1:], outs):
        ref[...] = decoded(wt_ref, q, rounded, ref.shape).astype(BF)


def own_body(wt_ref, coded_ref, x_ref, own_ref, loss_ref, *last):
    coded = coded_ref[...]
    rounded = coded.astype(BF)
    batch = coded.shape[-1]
    for ref in last:
        ref[...] = decoded(wt_ref, spilled()[2], rounded, ref.shape)
    own_ref[...] = decoded(wt_ref, 0, rounded, own_ref.shape) - x_ref[...].astype(F32)
    root = jnp.sqrt(smooth_eps + coded * coded)
    loss_ref[...] = sparsity_weight * jnp.sum(root.reshape(UNITS // 8, 8, batch), 0)


def join_body(last, passed, out_ref):
    out_ref[...] = (last[...] + passed[...].astype(F32)).astype(BF)


def error_body(own, sp, *refs):
    parts, (e_ref, loss_ref) = refs[:-2], refs[-2:]
    batch = own.shape[-1]
    total = sp[...]
    for ch in range(3):
        err = own[ch]
        for ref in parts:
            err = err + ref[ch].astype(F32)
        e_ref[ch] = err.astype(BF)
        total = total + jnp.sum((err * err).reshape(QUAD // 8, 8, batch), 0)
    loss_ref[...] = total


def ready_body(coded_ref, e_ref, x_ref, *refs):
    slots, (left_ref, pull_ref, xe, copy_ref) = refs[:-4], refs[-4:]
    copy_ref[...] = e_ref[...]
    coded = coded_ref[...]
    left_ref[...] = (2.0 * coded).astype(BF)
    pull_ref[...] = sparsity_weight * coded / jnp.sqrt(smooth_eps + coded * coded)
    place(xe, x_ref, slots)


def gradient_rows(half, wd_ref, left_ref, pull_ref, con_ref, st_ref, ex, gd, gs, out):
    at = pl.multiple_of(half * HALF, HALF)
    rows = pl.ds(at, HALF)
    batch = left_ref.shape[-1]
    e_all = ex[:, :, :batch].reshape(3 * PLANE, batch)
    enc = jnp.dot(wd_ref[rows, :], e_all, preferred_element_type=F32)
    left = left_ref[rows, :].astype(F32)
    right = 2.0 * enc + pull_ref[rows, :]
    con = con_ref[rows, :]
    shift = half * (SIDE_POS // 2 * STRIDE * SPAN)
    out[...] = jnp.zeros((HALF, PAD_IN), F32)
    for ch in range(3):
        opened = con[:, ch : ch + 1]
        both = jnp.concatenate([(left * opened).astype(BF), (right * opened).astype(BF)], 1)
        gd[...] = lax.dot_general(
            both, ex[ch], (((1,), (1,)), ((), ())), preferred_element_type=F32
        )
        for u, lead, shifts in positions(SIDE_POS // 2):
            parts = []
            lanes = pl.ds(pl.multiple_of(lead + shift, LANES), PAD_STRIP)
            for h, s in enumerate(shifts):
                blk = gd[u + h * MAPS : u + (h + 1) * MAPS, lanes]
                parts.append(pltpu.roll(blk, PAD_STRIP - s, 1) if s else blk)
            gs[u : u + 2 * MAPS, :] = jnp.concatenate(parts, 0).astype(BF)
        cols = slice(ch * STEP_IN, ch * STEP_IN + GRAB)
        out[:, cols] = out[:, cols] + jnp.dot(gs[...], st_ref[ch], preferred_element_type=F32)


def away_body(wd_ref, left_ref, pull_ref, con_ref, st_ref, xe, e_ref, *refs):
    slots, (send_ref, ex, tmp, gd, gs, out) = refs[:-6], refs[-6:]
    batch = e_ref.shape[-1]
    place(tmp, e_ref, slots)
    for ch in range(3):
        ex[ch, :, :batch] = tmp[ch].reshape(PLANE, batch)
        ex[ch, :, batch:] = xe[ch].reshape(PLANE, batch)
    core = lax.axis_index("dp") % 2
    gradient_rows(1 - core, wd_ref, left_ref, pull_ref, con_ref, st_ref, ex, gd, gs, out)
    send_ref[...] = out[...].astype(BF)


def home_body(wd_ref, left_ref, pull_ref, con_ref, st_ref, ex, keep_ref, gd, gs):
    core = lax.axis_index("dp") % 2
    gradient_rows(core, wd_ref, left_ref, pull_ref, con_ref, st_ref, ex, gd, gs, keep_ref)


def pair_body(keep, got, *refs):
    own_ref, sends, scr = refs[0], refs[1:-1], refs[-1]
    rows = own_ref.shape[0]
    scr[...] = keep[...] + got[...].astype(F32)
    chip = lax.axis_index("dp") // 2
    own_ref[...] = scr[pl.ds(pl.multiple_of(chip * rows, rows), rows), :]
    for x, ref in enumerate(sends):
        at = pl.multiple_of((chip ^ (x + 1)) * rows, rows)
        ref[...] = scr[pl.ds(at, rows), :].astype(BF)


def total_of(value):
    return jnp.sum(jnp.sum(value, 0, keepdims=True), 1, keepdims=True)


def shard_body(own, *refs):
    got, loss, shard_ref, tally_ref = refs[:-3], refs[-3], refs[-2], refs[-1]
    total = own[...]
    for ref in got:
        total = total + ref[...].astype(F32)
    shard_ref[...] = total.astype(BF)
    lane = lax.broadcasted_iota(jnp.int32, (8, LANES), 1)
    squares = total_of(total * total)
    tally_ref[...] = jnp.where(lane == 0, total_of(loss[...]), jnp.where(lane == 1, squares, 0.0))


def sum_body(*refs):
    total = refs[0][...]
    for ref in refs[1:-1]:
        total = total + ref[...]
    refs[-1][...] = total


def gather_body(own, *refs):
    got, half_ref = refs[:-1], refs[-1]
    rows = own.shape[0]
    chip = lax.axis_index("dp") // 2
    half_ref[pl.ds(pl.multiple_of(chip * rows, rows), rows), :] = own[...]
    for x, ref in enumerate(got):
        at = pl.multiple_of((chip ^ (x + 1)) * rows, rows)
        half_ref[pl.ds(at, rows), :] = ref[...]


def finish_body(entries, frames_total, mine, other, *refs):
    tallies, up_ref, loss_ref = refs[:-2], refs[-2], refs[-1]
    tally = tallies[0][...]
    for ref in tallies[1:]:
        tally = tally + ref[...]
    lane = lax.broadcasted_iota(jnp.int32, (1, LANES), 1)
    row = tally[:1]
    square = total_of(jnp.where(lane == 1, row, 0.0))
    factor = -lax.rsqrt(square / entries + guard_eps)
    core = lax.axis_index("dp") % 2
    for half, ref in ((core, mine), (1 - core, other)):
        at = pl.multiple_of(half * HALF, HALF)
        up_ref[pl.ds(at, HALF), :] = (ref[:, :INPUTS].astype(F32) * factor).astype(BF)
    loss_ref[0, 0] = jnp.sum(jnp.where(lane == 0, row, 0.0)) / frames_total


def local(frames, weights, connect):
    batch = frames.shape[-1]
    n_tile = lax.axis_size("tile")
    n_dp = lax.axis_size("dp")
    chips = n_dp // 2
    sds = jax.ShapeDtypeStruct
    mac = 2 * UNITS * 3 * PLANE * batch
    quad = (3, TILE_PX, TILE_PX, batch)
    units = (UNITS, batch)
    plane = (3, SPAN, SPAN, batch)
    to_first, to_second, to_third, onward = routes(n_tile)
    relay = onward is not None

    def spread_out(now, later):
        first = send(now, "tile", to_first)
        second = send(later, "tile", to_second)
        third = send(later, "tile", to_third)
        if not relay:
            return [first, second, third]
        return [first, second, third, send(first, "tile", onward)]

    x0 = frames[0]
    con = connect.reshape(UNITS, 3).astype(F32)
    wp, x_late = kernel_call(
        stage_body, (sds((UNITS, PAD_IN), BF), sds(quad, BF)), n_in=2, flops=mac // 64
    )(weights.reshape(UNITS, INPUTS), x0)
    xs = spread_out(x0, x_late if relay else x0)
    wd, wt, st = kernel_call(
        expand_body,
        (sds((UNITS, 3 * PLANE), BF), sds((4, 3 * QUAD, UNITS), BF), sds((3, PAD_STRIP, GRAB), BF)),
        [pltpu.VMEM((UNITS, PAD_STRIP), F32), pltpu.VMEM((GRAB, PAD_STRIP), BF)],
        n_in=2, flops=4 * mac,
    )(wp, con)

    coded, s1 = kernel_call(
        coded_body,
        (sds(units, F32), sds(quad, BF)),
        [pltpu.VMEM(plane, BF)],
        n_in=3 + len(xs), flops=mac,
    )(x0, *xs, wd, wt)
    parts = []
    if relay:
        passed = send(s1, "tile", [(0, 1), (3, 2)])
    parts.append(send(s1, "tile", [(1, 2), (2, 1)] if relay else flip_all(to_third)))
    s2, *s3 = kernel_call(
        spill_body,
        (sds(quad, BF),) * (1 if relay else 2),
        n_in=2, flops=mac // 4,
    )(wt, coded)
    parts.append(send(s2, "tile", flip_all(to_second)))
    own, sparse, *last = kernel_call(
        own_body,
        (sds(quad, F32), sds((8, batch), F32)) + (sds(quad, F32),) * relay,
        n_in=3, flops=mac // 2,
    )(wt, coded, x0)
    if relay:
        s3 = kernel_call(join_body, (sds(quad, BF),), n_in=2, flops=mac // 64)(last[0], passed)
    parts.append(send(s3[0], "tile", flip_all(to_first)))
    e0, loss_part = kernel_call(
        error_body, (sds(quad, BF), sds((8, batch), F32)), n_in=2 + len(parts), flops=mac // 32
    )(own, sparse, *parts)

    left, pull, xe, e_late = kernel_call(
        ready_body,
        (sds(units, BF), sds(units, F32), sds(plane, BF), sds(quad, BF)),
        n_in=3 + len(xs), flops=mac // 16,
    )(coded, e0, x0, *xs)
    es = spread_out(e0, e_late if relay else e0)

    half = (HALF, PAD_IN)
    work = [pltpu.VMEM((HALF, PLANE), F32), pltpu.VMEM((HALF, PAD_STRIP), BF)]
    away, ex = kernel_call(
        away_body,
        (sds(half, BF), sds((3, PLANE, 2 * batch), BF)),
        [pltpu.VMEM(plane, BF)] + work + [pltpu.VMEM(half, F32)],
        n_in=7 + len(es), flops=2 * mac,
    )(wd, left, pull, con, st, xe, e0, *es)
    got = send(away, "dp", flips(n_dp, 1))
    (keep,) = kernel_call(
        home_body, (sds(half, F32),), work, n_in=6, flops=2 * mac
    )(wd, left, pull, con, st, ex)

    rows = HALF // chips
    shard = sds((rows, PAD_IN), BF)
    split = kernel_call(
        pair_body,
        (sds((rows, PAD_IN), F32),) + (shard,) * (chips - 1),
        [pltpu.VMEM(half, F32)],
        n_in=2, flops=mac // 32,
    )(keep, got)
    arrived = [send(v, "dp", flips(n_dp, 2 * (x + 1))) for x, v in enumerate(split[1:])]
    line = sds((8, LANES), F32)
    mine, tally = kernel_call(shard_body, (shard, line), n_in=chips + 1, flops=mac // 64)(
        split[0], *arrived, loss_part
    )

    def add_up(*values):
        return kernel_call(sum_body, (line,), n_in=len(values), flops=mac // 64)(*values)[0]

    across = [flips(n_dp, 2 * x) for x in range(1, chips)]
    told = in_turn([tally] * (chips - 1), "dp", across)
    others = in_turn([mine] * (chips - 1), "dp", across)
    tally = add_up(tally, *told)
    tally = add_up(tally, send(tally, "dp", flips(n_dp, 1)))
    tallies = in_turn([tally] * (n_tile - 1), "tile", [ring(n_tile, s) for s in range(1, n_tile)])
    tally = add_up(tally)
    (mine_half,) = kernel_call(
        gather_body, (sds(half, BF),), n_in=chips, flops=mac // 64
    )(mine, *others)
    other_half = send(mine_half, "dp", flips(n_dp, 1))

    entries = n_tile * POS * MAPS * INPUTS
    update, loss = kernel_call(
        functools.partial(finish_body, float(entries), float(batch * n_dp)),
        (sds((UNITS, INPUTS), BF), sds((1, 1), F32)),
        n_in=2 + n_tile, flops=mac // 32, scalar_out=True,
    )(mine_half, other_half, tally, *tallies)
    return update.reshape(1, POS, MAPS, INPUTS), loss.reshape(())


def solution(mesh):
    placed = (
        P("tile", None, None, None, "dp"),
        P("tile", None, None, None),
        P("tile", None, None, None),
    )
    return jax.shard_map(
        local,
        mesh=mesh,
        in_specs=placed,
        out_specs=(P("tile", None, None, None), P()),
        check_vma=False,
    )
```

```python
import functools
import math

import jax
import jax.numpy as jnp
from jax import lax
from jax.experimental import pallas as pl
from jax.experimental.pallas import tpu as pltpu
from jax.sharding import PartitionSpec as P


FIELD = 18
MAPS = 8
STRIDE = 2
TILE_PX = 16
INPUTS = 972
HALO = 16
POS = 64
SPAN = TILE_PX + HALO
SIDE_POS = TILE_PX // STRIDE
UNITS = POS * MAPS
HALF = UNITS // 2
PLANE = SPAN * SPAN
QUAD = TILE_PX * TILE_PX
PATCH = FIELD * FIELD
LANES = 128
PAD_IN = -(-INPUTS // LANES) * LANES
PAD_STRIP = -(-FIELD * SPAN // LANES) * LANES
GRAB = 512
STEP_IN = 256

sparsity_weight = 1.0
smooth_eps = 0.01
guard_eps = 1e-06


BF = jnp.bfloat16
F32 = jnp.float32
VMEM_CAP = 24 * 1024 * 1024
RELAY_TILES = 4


def send(value, axis, pairs):
    return lax.ppermute(value, axis, pairs)


def ring(count, steps):
    return [(s, (s + steps) % count) for s in range(count)]


def flips(count, flip):
    return [(s, s ^ flip) for s in range(count)]


def in_turn(values, axis, routes):
    out = []
    for value, pairs in zip(values, routes):
        out.append(send(value, axis, pairs))
    return out


def flip_all(pairs):
    return [(b, a) for a, b in pairs]


def routes(n_tile):
    side = math.isqrt(n_tile)
    if n_tile == RELAY_TILES:
        return (
            [(0, 2), (3, 1), (1, 0), (2, 3)],
            [(1, 3), (2, 0), (0, 1), (3, 2)],
            [(1, 2), (2, 1), (0, 0), (3, 3)],
            [(2, 3), (1, 0), (0, 1), (3, 2)],
        )
    return ring(n_tile, -1), ring(n_tile, -side), ring(n_tile, -side - 1), None


def inner_tile():
    t = lax.axis_index("tile")
    return (t == 1) | (t == 2)


def quadrants():
    if lax.axis_size("tile") != RELAY_TILES:
        return 1, 2, 3
    t = lax.axis_index("tile")
    first = jnp.where(inner_tile(), 2, jnp.where(t == 0, 1, 3))
    second = jnp.where(t == 1, 3, jnp.where(t == 2, 1, 2))
    third = jnp.where(t % 2 == 0, 3, 1)
    return first, second, third


def spilled():
    return quadrants()[::-1]


def kernel_call(body, outs, scratch=(), n_in=0, flops=0, scalar_out=False):
    places = [pltpu.VMEM] * (len(outs) - scalar_out) + [pltpu.SMEM] * scalar_out
    return pl.pallas_call(
        body,
        out_shape=outs,
        in_specs=[pl.BlockSpec(memory_space=pltpu.VMEM)] * n_in,
        out_specs=tuple(pl.BlockSpec(memory_space=place) for place in places),
        scratch_shapes=list(scratch),
        compiler_params=pltpu.CompilerParams(vmem_limit_bytes=VMEM_CAP),
        cost_estimate=pl.CostEstimate(flops=flops, transcendentals=0, bytes_accessed=flops // 256),
    )


def positions(rows):
    for i in range(rows):
        for j in range(0, SIDE_POS, 2):
            lead = i * STRIDE * SPAN // LANES * LANES
            rest = i * STRIDE * SPAN - lead
            yield (i * SIDE_POS + j) * MAPS, lead, (rest + STRIDE * j, rest + STRIDE * (j + 1))


def place(dst, own, slots):
    def put(q, ref):
        top = pl.multiple_of(q // 2 * TILE_PX, TILE_PX)
        left = pl.multiple_of(q % 2 * TILE_PX, TILE_PX)
        for ch in range(3):
            dst[ch, pl.ds(top, TILE_PX), pl.ds(left, TILE_PX), :] = ref[ch]

    first, second, third = quadrants()
    put(0, own)
    put(first, slots[0])
    put(second, slots[1])
    if len(slots) == 3:
        put(third, slots[2])
    else:
        inner = inner_tile()
        pl.when(inner)(lambda: put(third, slots[2]))
        pl.when(jnp.logical_not(inner))(lambda: put(third, slots[3]))


def stage_body(w_ref, x_ref, wp_ref, copy_ref):
    copy_ref[...] = x_ref[...]
    wp_ref[:, PAD_IN - LANES :] = jnp.zeros((UNITS, LANES), BF)
    wp_ref[:, :INPUTS] = w_ref[...]


def expand_body(wp_ref, con_ref, wd_ref, wt_ref, st_ref, v_ref, s_ref):
    def wanted(shape, axis):
        n = lax.broadcasted_iota(jnp.int32, shape, axis)
        row, col = n // SPAN, n % SPAN
        return (col < FIELD) & (row < FIELD), row * FIELD + col

    inside, source = wanted((1, PAD_STRIP), 1)
    inside_t, source_t = wanted((PAD_STRIP, 1), 0)
    k = lax.broadcasted_iota(jnp.int32, (GRAB, PAD_STRIP), 0)
    k_t = lax.broadcasted_iota(jnp.int32, (PAD_STRIP, GRAB), 1)
    for ch in range(3):
        skip = ch * (PATCH - STEP_IN)
        want = jnp.where(inside, source + skip, -1)
        s_ref[...] = jnp.where(k == want, 1.0, 0.0).astype(BF)
        want = jnp.where(inside_t, source_t + skip, -1)
        st_ref[ch] = jnp.where(k_t == want, 1.0, 0.0).astype(BF)
        v = jnp.dot(
            wp_ref[:, ch * STEP_IN : ch * STEP_IN + GRAB], s_ref[...], preferred_element_type=F32
        )
        v_ref[...] = v * con_ref[:, ch : ch + 1]
        base = ch * PLANE
        for u, lead, shifts in positions(SIDE_POS):
            parts = []
            for h, s in enumerate(shifts):
                blk = v_ref[u + h * MAPS : u + (h + 1) * MAPS, :]
                parts.append(pltpu.roll(blk, s, 1) if s else blk)
            rows = slice(u, u + 2 * MAPS)
            if lead:
                wd_ref[rows, base : base + lead] = jnp.zeros((2 * MAPS, lead), BF)
            end = lead + PAD_STRIP
            wd_ref[rows, base + lead : base + end] = jnp.concatenate(parts, 0).astype(BF)
            if end < PLANE:
                wd_ref[rows, base + end : base + PLANE] = jnp.zeros((2 * MAPS, PLANE - end), BF)
        for at in range(0, PLANE, LANES):
            flipped = wd_ref[:, base + at : base + at + LANES].T
            for sub in range(0, LANES, TILE_PX):
                row, col = (at + sub) // SPAN, (at + sub) % SPAN
                q = row // TILE_PX * 2 + col // TILE_PX
                to = ch * QUAD + row % TILE_PX * TILE_PX
                wt_ref[q, to : to + TILE_PX, :] = flipped[sub : sub + TILE_PX]


def decoded(wt_ref, q, rounded, shape):
    return jnp.dot(wt_ref[q], rounded, preferred_element_type=F32).reshape(shape)


def coded_body(x_ref, *refs):
    slots, (wd_ref, wt_ref, coded_ref, out_ref, xe) = refs[:-5], refs[-5:]
    place(xe, x_ref, slots)
    batch = x_ref.shape[-1]
    coded = jnp.dot(wd_ref[...], xe[...].reshape(3 * PLANE, batch), preferred_element_type=F32)
    coded_ref[...] = coded
    out_ref[...] = decoded(wt_ref, spilled()[0], coded.astype(BF), out_ref.shape).astype(BF)


def spill_body(wt_ref, coded_ref, *outs):
    rounded = coded_ref[...].astype(BF)
    for q, ref in zip(spilled()[1:], outs):
        ref[...] = decoded(wt_ref, q, rounded, ref.shape).astype(BF)


def own_body(wt_ref, coded_ref, x_ref, own_ref, loss_ref, *last):
    coded = coded_ref[...]
    rounded = coded.astype(BF)
    batch = coded.shape[-1]
    for ref in last:
        ref[...] = decoded(wt_ref, spilled()[2], rounded, ref.shape)
    own_ref[...] = decoded(wt_ref, 0, rounded, own_ref.shape) - x_ref[...].astype(F32)
    root = jnp.sqrt(smooth_eps + coded * coded)
    loss_ref[...] = sparsity_weight * jnp.sum(root.reshape(UNITS // 8, 8, batch), 0)


def join_body(last, passed, out_ref):
    out_ref[...] = (last[...] + passed[...].astype(F32)).astype(BF)


def error_body(own, sp, *refs):
    parts, (e_ref, loss_ref) = refs[:-2], refs[-2:]
    batch = own.shape[-1]
    total = sp[...]
    for ch in range(3):
        err = own[ch]
        for ref in parts:
            err = err + ref[ch].astype(F32)
        e_ref[ch] = err.astype(BF)
        total = total + jnp.sum((err * err).reshape(QUAD // 8, 8, batch), 0)
    loss_ref[...] = total


def ready_body(coded_ref, e_ref, x_ref, *refs):
    slots, (left_ref, pull_ref, xe, copy_ref) = refs[:-4], refs[-4:]
    copy_ref[...] = e_ref[...]
    coded = coded_ref[...]
    left_ref[...] = (2.0 * coded).astype(BF)
    pull_ref[...] = sparsity_weight * coded / jnp.sqrt(smooth_eps + coded * coded)
    place(xe, x_ref, slots)


def gradient_rows(half, wd_ref, left_ref, pull_ref, con_ref, st_ref, ex, gd, gs, acc, out):
    at = pl.multiple_of(half * HALF, HALF)
    rows = pl.ds(at, HALF)
    batch = left_ref.shape[-1]
    e_all = ex[:, :, :, :batch].reshape(3 * PLANE, batch)
    enc = jnp.dot(wd_ref[rows, :], e_all, preferred_element_type=F32)
    left = left_ref[rows, :].astype(F32)
    right = 2.0 * enc + pull_ref[rows, :]
    con = con_ref[rows, :]
    shift = half * (SIDE_POS // 2 * STRIDE * SPAN)
    for ch in range(3):
        opened = con[:, ch : ch + 1]
        both = jnp.concatenate([(left * opened).astype(BF), (right * opened).astype(BF)], 1)
        gd[ch][...] = lax.dot_general(
            both,
            ex[ch].reshape(PLANE, 2 * batch),
            (((1,), (1,)), ((), ())),
            preferred_element_type=F32,
        )
    for ch in range(3):
        for u, lead, shifts in positions(SIDE_POS // 2):
            parts = []
            lanes = pl.ds(pl.multiple_of(lead + shift, LANES), PAD_STRIP)
            for h, s in enumerate(shifts):
                blk = gd[ch][u + h * MAPS : u + (h + 1) * MAPS, lanes]
                parts.append(pltpu.roll(blk, PAD_STRIP - s, 1) if s else blk)
            gs[ch][u : u + 2 * MAPS, :] = jnp.concatenate(parts, 0).astype(BF)
        acc[ch][...] = jnp.dot(gs[ch][...], st_ref[ch], preferred_element_type=F32)
    for at in range(0, PAD_IN, STEP_IN):
        first = at // STEP_IN
        parts = [acc[ch][:, at - ch * STEP_IN : at - ch * STEP_IN + STEP_IN] for ch in (first, first - 1) if 0 <= ch < 3]
        out[:, at : at + STEP_IN] = sum(parts[1:], parts[0]).astype(out.dtype)


def away_body(wd_ref, left_ref, pull_ref, con_ref, st_ref, xe, e_ref, *refs):
    slots, (send_ref, ex), work = refs[:-11], refs[-11:-9], refs[-9:]
    batch = e_ref.shape[-1]
    place(ex.at[:, :, :, :batch], e_ref, slots)
    for ch in range(3):
        ex[ch, :, :, batch:] = xe[ch]
    core = lax.axis_index("dp") % 2
    gradient_rows(
        1 - core, wd_ref, left_ref, pull_ref, con_ref, st_ref, ex, work[:3], work[3:6], work[6:], send_ref
    )


def home_body(wd_ref, left_ref, pull_ref, con_ref, st_ref, ex, keep_ref, *work):
    core = lax.axis_index("dp") % 2
    gradient_rows(
        core, wd_ref, left_ref, pull_ref, con_ref, st_ref, ex, work[:3], work[3:6], work[6:], keep_ref
    )


def pair_body(keep, got, *refs):
    own_ref, sends, scr = refs[0], refs[1:-1], refs[-1]
    rows = own_ref.shape[0]
    scr[...] = keep[...] + got[...].astype(F32)
    chip = lax.axis_index("dp") // 2
    own_ref[...] = scr[pl.ds(pl.multiple_of(chip * rows, rows), rows), :]
    for x, ref in enumerate(sends):
        at = pl.multiple_of((chip ^ (x + 1)) * rows, rows)
        ref[...] = scr[pl.ds(at, rows), :].astype(BF)


def total_of(value):
    return jnp.sum(jnp.sum(value, 0, keepdims=True), 1, keepdims=True)


def shard_body(own, *refs):
    got, loss, shard_ref, tally_ref = refs[:-3], refs[-3], refs[-2], refs[-1]
    total = own[...]
    for ref in got:
        total = total + ref[...].astype(F32)
    shard_ref[...] = total.astype(BF)
    lane = lax.broadcasted_iota(jnp.int32, (8, LANES), 1)
    squares = total_of(total * total)
    tally_ref[...] = jnp.where(lane == 0, total_of(loss[...]), jnp.where(lane == 1, squares, 0.0))


def sum_body(*refs):
    total = refs[0][...]
    for ref in refs[1:-1]:
        total = total + ref[...]
    refs[-1][...] = total


def gather_body(own, *refs):
    got, half_ref = refs[:-1], refs[-1]
    rows = own.shape[0]
    chip = lax.axis_index("dp") // 2
    half_ref[pl.ds(pl.multiple_of(chip * rows, rows), rows), :] = own[...]
    for x, ref in enumerate(got):
        at = pl.multiple_of((chip ^ (x + 1)) * rows, rows)
        half_ref[pl.ds(at, rows), :] = ref[...]


def finish_body(entries, frames_total, mine, other, *refs):
    tallies, up_ref, loss_ref = refs[:-2], refs[-2], refs[-1]
    tally = tallies[0][...]
    for ref in tallies[1:]:
        tally = tally + ref[...]
    lane = lax.broadcasted_iota(jnp.int32, (1, LANES), 1)
    row = tally[:1]
    square = total_of(jnp.where(lane == 1, row, 0.0))
    factor = -lax.rsqrt(square / entries + guard_eps)
    core = lax.axis_index("dp") % 2
    for half, ref in ((core, mine), (1 - core, other)):
        at = pl.multiple_of(half * HALF, HALF)
        up_ref[pl.ds(at, HALF), :] = (ref[:, :INPUTS].astype(F32) * factor).astype(BF)
    loss_ref[0, 0] = jnp.sum(jnp.where(lane == 0, row, 0.0)) / frames_total


def local(frames, weights, connect):
    batch = frames.shape[-1]
    n_tile = lax.axis_size("tile")
    n_dp = lax.axis_size("dp")
    chips = n_dp // 2
    sds = jax.ShapeDtypeStruct
    mac = 2 * UNITS * 3 * PLANE * batch
    quad = (3, TILE_PX, TILE_PX, batch)
    units = (UNITS, batch)
    plane = (3, SPAN, SPAN, batch)
    to_first, to_second, to_third, onward = routes(n_tile)
    relay = onward is not None

    def spread_out(now, later):
        first = send(now, "tile", to_first)
        second = send(later, "tile", to_second)
        third = send(later, "tile", to_third)
        if not relay:
            return [first, second, third]
        return [first, second, third, send(first, "tile", onward)]

    x0 = frames[0]
    con = connect.reshape(UNITS, 3).astype(F32)
    wp, _ = kernel_call(
        stage_body, (sds((UNITS, PAD_IN), BF), sds(quad, BF)), n_in=2, flops=mac // 64
    )(weights.reshape(UNITS, INPUTS), x0)
    xs = spread_out(x0, x0)
    wd, wt, st = kernel_call(
        expand_body,
        (sds((UNITS, 3 * PLANE), BF), sds((4, 3 * QUAD, UNITS), BF), sds((3, PAD_STRIP, GRAB), BF)),
        [pltpu.VMEM((UNITS, PAD_STRIP), F32), pltpu.VMEM((GRAB, PAD_STRIP), BF)],
        n_in=2, flops=4 * mac,
    )(wp, con)

    coded, s1 = kernel_call(
        coded_body,
        (sds(units, F32), sds(quad, BF)),
        [pltpu.VMEM(plane, BF)],
        n_in=3 + len(xs), flops=mac,
    )(x0, *xs, wd, wt)
    parts = []
    if relay:
        passed = send(s1, "tile", [(0, 1), (3, 2)])
    parts.append(send(s1, "tile", [(1, 2), (2, 1)] if relay else flip_all(to_third)))
    s2, *s3 = kernel_call(
        spill_body,
        (sds(quad, BF),) * (1 if relay else 2),
        n_in=2, flops=mac // 4,
    )(wt, coded)
    parts.append(send(s2, "tile", flip_all(to_second)))
    own, sparse, *last = kernel_call(
        own_body,
        (sds(quad, F32), sds((8, batch), F32)) + (sds(quad, F32),) * relay,
        n_in=3, flops=mac // 2,
    )(wt, coded, x0)
    if relay:
        s3 = kernel_call(join_body, (sds(quad, BF),), n_in=2, flops=mac // 64)(last[0], passed)
    parts.append(send(s3[0], "tile", flip_all(to_first)))
    e0, loss_part = kernel_call(
        error_body, (sds(quad, BF), sds((8, batch), F32)), n_in=2 + len(parts), flops=mac // 32
    )(own, sparse, *parts)

    left, pull, xe, e_late = kernel_call(
        ready_body,
        (sds(units, BF), sds(units, F32), sds(plane, BF), sds(quad, BF)),
        n_in=3 + len(xs), flops=mac // 16,
    )(coded, e0, x0, *xs)
    es = spread_out(e0, e_late if relay else e0)

    half = (HALF, PAD_IN)
    work = [pltpu.VMEM((HALF, PLANE), F32)] * 3
    work += [pltpu.VMEM((HALF, PAD_STRIP), BF)] * 3 + [pltpu.VMEM((HALF, GRAB), F32)] * 3
    away, ex = kernel_call(
        away_body,
        (sds(half, BF), sds((3, SPAN, SPAN, 2 * batch), BF)),
        work,
        n_in=7 + len(es), flops=2 * mac,
    )(wd, left, pull, con, st, xe, e0, *es)
    got = send(away, "dp", flips(n_dp, 1))
    (keep,) = kernel_call(
        home_body, (sds(half, F32),), work, n_in=6, flops=2 * mac
    )(wd, left, pull, con, st, ex)

    rows = HALF // chips
    shard = sds((rows, PAD_IN), BF)
    split = kernel_call(
        pair_body,
        (sds((rows, PAD_IN), F32),) + (shard,) * (chips - 1),
        [pltpu.VMEM(half, F32)],
        n_in=2, flops=mac // 32,
    )(keep, got)
    arrived = [send(v, "dp", flips(n_dp, 2 * (x + 1))) for x, v in enumerate(split[1:])]
    line = sds((8, LANES), F32)
    mine, tally = kernel_call(shard_body, (shard, line), n_in=chips + 1, flops=mac // 64)(
        split[0], *arrived, loss_part
    )

    def add_up(*values):
        return kernel_call(sum_body, (line,), n_in=len(values), flops=mac // 64)(*values)[0]

    across = [flips(n_dp, 2 * x) for x in range(1, chips)]
    told = in_turn([tally] * (chips - 1), "dp", across)
    others = in_turn([mine] * (chips - 1), "dp", across)
    tally = add_up(tally, *told)
    tally = add_up(tally, send(tally, "dp", flips(n_dp, 1)))
    tallies = in_turn([tally] * (n_tile - 1), "tile", [ring(n_tile, s) for s in range(1, n_tile)])
    tally = add_up(tally)
    (mine_half,) = kernel_call(
        gather_body, (sds(half, BF),), n_in=chips, flops=mac // 64
    )(mine, *others)
    other_half = send(mine_half, "dp", flips(n_dp, 1))

    entries = n_tile * POS * MAPS * INPUTS
    update, loss = kernel_call(
        functools.partial(finish_body, float(entries), float(batch * n_dp)),
        (sds((UNITS, INPUTS), BF), sds((1, 1), F32)),
        n_in=2 + n_tile, flops=mac // 32, scalar_out=True,
    )(mine_half, other_half, tally, *tallies)
    return update.reshape(1, POS, MAPS, INPUTS), loss.reshape(())


def solution(mesh):
    placed = (
        P("tile", None, None, None, "dp"),
        P("tile", None, None, None),
        P("tile", None, None, None),
    )
    return jax.shard_map(
        local,
        mesh=mesh,
        in_specs=placed,
        out_specs=(P("tile", None, None, None), P()),
        check_vma=False,
    )
```

```python
import functools
import math

import jax
import jax.numpy as jnp
from jax import lax
from jax.experimental import pallas as pl
from jax.experimental.pallas import tpu as pltpu
from jax.sharding import PartitionSpec as P


FIELD = 18
MAPS = 8
STRIDE = 2
TILE_PX = 16
INPUTS = 972
HALO = 16
POS = 64
SPAN = TILE_PX + HALO
SIDE_POS = TILE_PX // STRIDE
UNITS = POS * MAPS
HALF = UNITS // 2
PLANE = SPAN * SPAN
QUAD = TILE_PX * TILE_PX
PATCH = FIELD * FIELD
LANES = 128
PAD_IN = -(-INPUTS // LANES) * LANES
PAD_STRIP = -(-FIELD * SPAN // LANES) * LANES
GRAB = 512
STEP_IN = 256

sparsity_weight = 1.0
smooth_eps = 0.01
guard_eps = 1e-06


BF = jnp.bfloat16
F32 = jnp.float32
VMEM_CAP = 24 * 1024 * 1024
RELAY_TILES = 4


def send(value, axis, pairs):
    return lax.ppermute(value, axis, pairs)


def ring(count, steps):
    return [(s, (s + steps) % count) for s in range(count)]


def flips(count, flip):
    return [(s, s ^ flip) for s in range(count)]


def in_turn(values, axis, routes):
    out = []
    for value, pairs in zip(values, routes):
        out.append(send(value, axis, pairs))
    return out


def flip_all(pairs):
    return [(b, a) for a, b in pairs]


def routes(n_tile):
    side = math.isqrt(n_tile)
    if n_tile == RELAY_TILES:
        return (
            [(0, 2), (3, 1), (1, 0), (2, 3)],
            [(1, 3), (2, 0), (0, 1), (3, 2)],
            [(1, 2), (2, 1), (0, 0), (3, 3)],
            [(2, 3), (1, 0), (0, 1), (3, 2)],
        )
    return ring(n_tile, -1), ring(n_tile, -side), ring(n_tile, -side - 1), None


def inner_tile():
    t = lax.axis_index("tile")
    return (t == 1) | (t == 2)


def quadrants():
    if lax.axis_size("tile") != RELAY_TILES:
        return 1, 2, 3
    t = lax.axis_index("tile")
    first = jnp.where(inner_tile(), 2, jnp.where(t == 0, 1, 3))
    second = jnp.where(t == 1, 3, jnp.where(t == 2, 1, 2))
    third = jnp.where(t % 2 == 0, 3, 1)
    return first, second, third


def spilled():
    return quadrants()[::-1]


def kernel_call(body, outs, scratch=(), n_in=0, flops=0, scalar_out=False):
    places = [pltpu.VMEM] * (len(outs) - scalar_out) + [pltpu.SMEM] * scalar_out
    return pl.pallas_call(
        body,
        out_shape=outs,
        in_specs=[pl.BlockSpec(memory_space=pltpu.VMEM)] * n_in,
        out_specs=tuple(pl.BlockSpec(memory_space=place) for place in places),
        scratch_shapes=list(scratch),
        compiler_params=pltpu.CompilerParams(vmem_limit_bytes=VMEM_CAP),
        cost_estimate=pl.CostEstimate(flops=flops, transcendentals=0, bytes_accessed=flops // 256),
    )


def positions(rows):
    for i in range(rows):
        for j in range(0, SIDE_POS, 2):
            lead = i * STRIDE * SPAN // LANES * LANES
            rest = i * STRIDE * SPAN - lead
            yield (i * SIDE_POS + j) * MAPS, lead, (rest + STRIDE * j, rest + STRIDE * (j + 1))


def place(dst, own, slots):
    def put(q, ref):
        top = pl.multiple_of(q // 2 * TILE_PX, TILE_PX)
        left = pl.multiple_of(q % 2 * TILE_PX, TILE_PX)
        for ch in range(3):
            dst[ch, pl.ds(top, TILE_PX), pl.ds(left, TILE_PX), :] = ref[ch]

    first, second, third = quadrants()
    put(0, own)
    put(first, slots[0])
    put(second, slots[1])
    if len(slots) == 3:
        put(third, slots[2])
    else:
        inner = inner_tile()
        pl.when(inner)(lambda: put(third, slots[2]))
        pl.when(jnp.logical_not(inner))(lambda: put(third, slots[3]))


def stage_body(w_ref, x_ref, wp_ref, copy_ref):
    copy_ref[...] = x_ref[...]
    wp_ref[:, PAD_IN - LANES :] = jnp.zeros((UNITS, LANES), BF)
    wp_ref[:, :INPUTS] = w_ref[...]


def expand_body(wp_ref, con_ref, wd_ref, wt_ref, st_ref, v_ref, s_ref):
    def wanted(shape, axis):
        n = lax.broadcasted_iota(jnp.int32, shape, axis)
        row, col = n // SPAN, n % SPAN
        return (col < FIELD) & (row < FIELD), row * FIELD + col

    inside, source = wanted((1, PAD_STRIP), 1)
    inside_t, source_t = wanted((PAD_STRIP, 1), 0)
    k = lax.broadcasted_iota(jnp.int32, (GRAB, PAD_STRIP), 0)
    k_t = lax.broadcasted_iota(jnp.int32, (PAD_STRIP, GRAB), 1)
    for ch in range(3):
        skip = ch * (PATCH - STEP_IN)
        want = jnp.where(inside, source + skip, -1)
        s_ref[...] = jnp.where(k == want, 1.0, 0.0).astype(BF)
        want = jnp.where(inside_t, source_t + skip, -1)
        st_ref[ch] = jnp.where(k_t == want, 1.0, 0.0).astype(BF)
        v = jnp.dot(
            wp_ref[:, ch * STEP_IN : ch * STEP_IN + GRAB], s_ref[...], preferred_element_type=F32
        )
        v_ref[...] = v * con_ref[:, ch : ch + 1]
        base = ch * PLANE
        for u, lead, shifts in positions(SIDE_POS):
            parts = []
            for h, s in enumerate(shifts):
                blk = v_ref[u + h * MAPS : u + (h + 1) * MAPS, :]
                parts.append(pltpu.roll(blk, s, 1) if s else blk)
            rows = slice(u, u + 2 * MAPS)
            if lead:
                wd_ref[rows, base : base + lead] = jnp.zeros((2 * MAPS, lead), BF)
            end = lead + PAD_STRIP
            wd_ref[rows, base + lead : base + end] = jnp.concatenate(parts, 0).astype(BF)
            if end < PLANE:
                wd_ref[rows, base + end : base + PLANE] = jnp.zeros((2 * MAPS, PLANE - end), BF)
        for at in range(0, PLANE, LANES):
            flipped = wd_ref[:, base + at : base + at + LANES].T
            for sub in range(0, LANES, TILE_PX):
                row, col = (at + sub) // SPAN, (at + sub) % SPAN
                q = row // TILE_PX * 2 + col // TILE_PX
                to = ch * QUAD + row % TILE_PX * TILE_PX
                wt_ref[q, to : to + TILE_PX, :] = flipped[sub : sub + TILE_PX]


def decoded(wt_ref, q, rounded, shape):
    return jnp.dot(wt_ref[q], rounded, preferred_element_type=F32).reshape(shape)


def coded_body(x_ref, *refs):
    slots, (wd_ref, wt_ref, coded_ref, out_ref, xe) = refs[:-5], refs[-5:]
    place(xe, x_ref, slots)
    batch = x_ref.shape[-1]
    coded = jnp.dot(wd_ref[...], xe[...].reshape(3 * PLANE, batch), preferred_element_type=F32)
    coded_ref[...] = coded
    out_ref[...] = decoded(wt_ref, spilled()[0], coded.astype(BF), out_ref.shape).astype(BF)


def spill_body(wt_ref, coded_ref, *outs):
    rounded = coded_ref[...].astype(BF)
    for q, ref in zip(spilled()[1:], outs):
        ref[...] = decoded(wt_ref, q, rounded, ref.shape).astype(BF)


def own_body(wt_ref, coded_ref, x_ref, own_ref, loss_ref, *last):
    coded = coded_ref[...]
    rounded = coded.astype(BF)
    batch = coded.shape[-1]
    for ref in last:
        ref[...] = decoded(wt_ref, spilled()[2], rounded, ref.shape)
    own_ref[...] = decoded(wt_ref, 0, rounded, own_ref.shape) - x_ref[...].astype(F32)
    root = jnp.sqrt(smooth_eps + coded * coded)
    loss_ref[...] = sparsity_weight * jnp.sum(root.reshape(UNITS // 8, 8, batch), 0)


def join_body(last, passed, out_ref):
    out_ref[...] = (last[...] + passed[...].astype(F32)).astype(BF)


def error_body(own, sp, *refs):
    parts, (e_ref, loss_ref) = refs[:-2], refs[-2:]
    batch = own.shape[-1]
    total = sp[...]
    for ch in range(3):
        err = own[ch]
        for ref in parts:
            err = err + ref[ch].astype(F32)
        e_ref[ch] = err.astype(BF)
        total = total + jnp.sum((err * err).reshape(QUAD // 8, 8, batch), 0)
    loss_ref[...] = total


def ready_body(coded_ref, e_ref, x_ref, *refs):
    slots, (left_ref, pull_ref, xe, copy_ref) = refs[:-4], refs[-4:]
    copy_ref[...] = e_ref[...]
    coded = coded_ref[...]
    left_ref[...] = (2.0 * coded).astype(BF)
    pull_ref[...] = sparsity_weight * coded / jnp.sqrt(smooth_eps + coded * coded)
    place(xe, x_ref, slots)


def gradient_rows(half, wd_ref, left_ref, pull_ref, con_ref, st_ref, ex, gd, gs, acc, out):
    at = pl.multiple_of(half * HALF, HALF)
    rows = pl.ds(at, HALF)
    batch = left_ref.shape[-1]
    e_all = ex[:, :, :, :batch].reshape(3 * PLANE, batch)
    enc = jnp.dot(wd_ref[rows, :], e_all, preferred_element_type=F32)
    left = left_ref[rows, :].astype(F32)
    right = 2.0 * enc + pull_ref[rows, :]
    con = con_ref[rows, :]
    shift = half * (SIDE_POS // 2 * STRIDE * SPAN)
    for ch in range(3):
        opened = con[:, ch : ch + 1]
        both = jnp.concatenate([(left * opened).astype(BF), (right * opened).astype(BF)], 1)
        gd[ch][...] = lax.dot_general(
            both,
            ex[ch].reshape(PLANE, 2 * batch),
            (((1,), (1,)), ((), ())),
            preferred_element_type=F32,
        )
    for ch in range(3):
        for u, lead, shifts in positions(SIDE_POS // 2):
            parts = []
            lanes = pl.ds(pl.multiple_of(lead + shift, LANES), PAD_STRIP)
            for h, s in enumerate(shifts):
                blk = gd[ch][u + h * MAPS : u + (h + 1) * MAPS, lanes]
                parts.append(pltpu.roll(blk, PAD_STRIP - s, 1) if s else blk)
            gs[ch][u : u + 2 * MAPS, :] = jnp.concatenate(parts, 0).astype(BF)
        acc[ch][...] = jnp.dot(gs[ch][...], st_ref[ch], preferred_element_type=F32)
    for at in range(0, PAD_IN, STEP_IN):
        first = at // STEP_IN
        parts = [acc[ch][:, at - ch * STEP_IN : at - ch * STEP_IN + STEP_IN] for ch in (first, first - 1) if 0 <= ch < 3]
        out[:, at : at + STEP_IN] = sum(parts[1:], parts[0]).astype(out.dtype)


def away_body(wd_ref, left_ref, pull_ref, con_ref, st_ref, xe, e_ref, *refs):
    slots, (send_ref, ex), work = refs[:-11], refs[-11:-9], refs[-9:]
    batch = e_ref.shape[-1]
    place(ex.at[:, :, :, :batch], e_ref, slots)
    for ch in range(3):
        ex[ch, :, :, batch:] = xe[ch]
    core = lax.axis_index("dp") % 2
    gradient_rows(
        1 - core, wd_ref, left_ref, pull_ref, con_ref, st_ref, ex, work[:3], work[3:6], work[6:], send_ref
    )


def home_body(wd_ref, left_ref, pull_ref, con_ref, st_ref, ex, keep_ref, *work):
    core = lax.axis_index("dp") % 2
    gradient_rows(
        core, wd_ref, left_ref, pull_ref, con_ref, st_ref, ex, work[:3], work[3:6], work[6:], keep_ref
    )


def pair_body(keep, got, *refs):
    own_ref, sends, scr = refs[0], refs[1:-1], refs[-1]
    rows = own_ref.shape[0]
    scr[...] = keep[...] + got[...].astype(F32)
    chip = lax.axis_index("dp") // 2
    own_ref[...] = scr[pl.ds(pl.multiple_of(chip * rows, rows), rows), :]
    for x, ref in enumerate(sends):
        at = pl.multiple_of((chip ^ (x + 1)) * rows, rows)
        ref[...] = scr[pl.ds(at, rows), :].astype(BF)


def total_of(value):
    return jnp.sum(jnp.sum(value, 0, keepdims=True), 1, keepdims=True)


def shard_body(own, *refs):
    got, loss, shard_ref, tally_ref = refs[:-3], refs[-3], refs[-2], refs[-1]
    total = own[...]
    for ref in got:
        total = total + ref[...].astype(F32)
    shard_ref[...] = total.astype(BF)
    lane = lax.broadcasted_iota(jnp.int32, (8, LANES), 1)
    squares = total_of(total * total)
    tally_ref[...] = jnp.where(lane == 0, total_of(loss[...]), jnp.where(lane == 1, squares, 0.0))


def sum_body(*refs):
    total = refs[0][...]
    for ref in refs[1:-1]:
        total = total + ref[...]
    refs[-1][...] = total


def gather_body(own, *refs):
    got, half_ref = refs[:-1], refs[-1]
    rows = own.shape[0]
    chip = lax.axis_index("dp") // 2
    half_ref[pl.ds(pl.multiple_of(chip * rows, rows), rows), :] = own[...]
    for x, ref in enumerate(got):
        at = pl.multiple_of((chip ^ (x + 1)) * rows, rows)
        half_ref[pl.ds(at, rows), :] = ref[...]


def finish_body(entries, frames_total, mine, other, *refs):
    tallies, up_ref, loss_ref = refs[:-2], refs[-2], refs[-1]
    tally = tallies[0][...]
    for ref in tallies[1:]:
        tally = tally + ref[...]
    lane = lax.broadcasted_iota(jnp.int32, (1, LANES), 1)
    row = tally[:1]
    square = total_of(jnp.where(lane == 1, row, 0.0))
    factor = -lax.rsqrt(square / entries + guard_eps)
    core = lax.axis_index("dp") % 2
    for half, ref in ((core, mine), (1 - core, other)):
        at = pl.multiple_of(half * HALF, HALF)
        up_ref[pl.ds(at, HALF), :] = (ref[:, :INPUTS].astype(F32) * factor).astype(BF)
    loss_ref[0, 0] = jnp.sum(jnp.where(lane == 0, row, 0.0)) / frames_total


def local(frames, weights, connect):
    batch = frames.shape[-1]
    n_tile = lax.axis_size("tile")
    n_dp = lax.axis_size("dp")
    chips = n_dp // 2
    sds = jax.ShapeDtypeStruct
    mac = 2 * UNITS * 3 * PLANE * batch
    quad = (3, TILE_PX, TILE_PX, batch)
    units = (UNITS, batch)
    plane = (3, SPAN, SPAN, batch)
    to_first, to_second, to_third, onward = routes(n_tile)
    relay = onward is not None

    def spread_out(now, later):
        first = send(now, "tile", to_first)
        second = send(later, "tile", to_second)
        third = send(later, "tile", to_third)
        if not relay:
            return [first, second, third]
        return [first, second, third, send(first, "tile", onward)]

    x0 = frames[0]
    con = connect.reshape(UNITS, 3).astype(F32)
    wp, _ = kernel_call(
        stage_body, (sds((UNITS, PAD_IN), BF), sds(quad, BF)), n_in=2, flops=mac // 64
    )(weights.reshape(UNITS, INPUTS), x0)
    xs = spread_out(x0, x0)
    wd, wt, st = kernel_call(
        expand_body,
        (sds((UNITS, 3 * PLANE), BF), sds((4, 3 * QUAD, UNITS), BF), sds((3, PAD_STRIP, GRAB), BF)),
        [pltpu.VMEM((UNITS, PAD_STRIP), F32), pltpu.VMEM((GRAB, PAD_STRIP), BF)],
        n_in=2, flops=4 * mac,
    )(wp, con)

    coded, s1 = kernel_call(
        coded_body,
        (sds(units, F32), sds(quad, BF)),
        [pltpu.VMEM(plane, BF)],
        n_in=3 + len(xs), flops=mac,
    )(x0, *xs, wd, wt)
    parts = []
    if relay:
        passed = send(s1, "tile", [(0, 1), (3, 2)])
    parts.append(send(s1, "tile", [(1, 2), (2, 1)] if relay else flip_all(to_third)))
    s2, *s3 = kernel_call(
        spill_body,
        (sds(quad, BF),) * (1 if relay else 2),
        n_in=2, flops=mac // 4,
    )(wt, coded)
    parts.append(send(s2, "tile", flip_all(to_second)))
    own, sparse, *last = kernel_call(
        own_body,
        (sds(quad, F32), sds((8, batch), F32)) + (sds(quad, F32),) * relay,
        n_in=3, flops=mac // 2,
    )(wt, coded, x0)
    if relay:
        s3 = kernel_call(join_body, (sds(quad, BF),), n_in=2, flops=mac // 64)(last[0], passed)
    parts.append(send(s3[0], "tile", flip_all(to_first)))
    e0, loss_part = kernel_call(
        error_body, (sds(quad, BF), sds((8, batch), F32)), n_in=2 + len(parts), flops=mac // 32
    )(own, sparse, *parts)

    left, pull, xe, e_late = kernel_call(
        ready_body,
        (sds(units, BF), sds(units, F32), sds(plane, BF), sds(quad, BF)),
        n_in=3 + len(xs), flops=mac // 16,
    )(coded, e0, x0, *xs)
    es = spread_out(e0, e_late if relay else e0)

    half = (HALF, PAD_IN)
    work = [pltpu.VMEM((HALF, PLANE), F32)] * 3
    work += [pltpu.VMEM((HALF, PAD_STRIP), BF)] * 3 + [pltpu.VMEM((HALF, GRAB), F32)] * 3
    away, ex = kernel_call(
        away_body,
        (sds(half, BF), sds((3, SPAN, SPAN, 2 * batch), BF)),
        work,
        n_in=7 + len(es), flops=2 * mac,
    )(wd, left, pull, con, st, xe, e0, *es)
    got = send(away, "dp", flips(n_dp, 1))
    (keep,) = kernel_call(
        home_body, (sds(half, F32),), work, n_in=6, flops=2 * mac
    )(wd, left, pull, con, st, ex)

    rows = HALF // chips
    shard = sds((rows, PAD_IN), BF)
    split = kernel_call(
        pair_body,
        (sds((rows, PAD_IN), F32),) + (shard,) * (chips - 1),
        [pltpu.VMEM(half, F32)],
        n_in=2, flops=mac // 32,
    )(keep, got)
    arrived = [send(v, "dp", flips(n_dp, 2 * (x + 1))) for x, v in enumerate(split[1:])]
    line = sds((8, LANES), F32)
    mine, tally = kernel_call(shard_body, (shard, line), n_in=chips + 1, flops=mac // 64)(
        split[0], *arrived, loss_part
    )

    def add_up(*values):
        return kernel_call(sum_body, (line,), n_in=len(values), flops=mac // 64)(*values)[0]

    across = [flips(n_dp, 2 * x) for x in range(1, chips)]
    others = in_turn([mine] * (chips - 1), "dp", across)
    flip = 2
    while flip < n_dp:
        told = send(tally, "dp", flips(n_dp, flip))
        tally = add_up(tally, told)
        flip *= 2
    told = send(tally, "dp", flips(n_dp, 1))
    tally = add_up(tally, told)
    tallies = in_turn([tally] * (n_tile - 1), "tile", [ring(n_tile, s) for s in range(1, n_tile)])
    tally = add_up(tally)
    (mine_half,) = kernel_call(
        gather_body, (sds(half, BF),), n_in=chips, flops=mac // 64
    )(mine, *others)
    other_half = send(mine_half, "dp", flips(n_dp, 1))

    entries = n_tile * POS * MAPS * INPUTS
    update, loss = kernel_call(
        functools.partial(finish_body, float(entries), float(batch * n_dp)),
        (sds((UNITS, INPUTS), BF), sds((1, 1), F32)),
        n_in=2 + n_tile, flops=mac // 32, scalar_out=True,
    )(mine_half, other_half, tally, *tallies)
    return update.reshape(1, POS, MAPS, INPUTS), loss.reshape(())


def solution(mesh):
    placed = (
        P("tile", None, None, None, "dp"),
        P("tile", None, None, None),
        P("tile", None, None, None),
    )
    return jax.shard_map(
        local,
        mesh=mesh,
        in_specs=placed,
        out_specs=(P("tile", None, None, None), P()),
        check_vma=False,
    )
```
